16 devices in a mesh: rep: 2 (over y, z), dp: 8 (over x, core).
Axes of the slice: x: 4, y: 2, z: 1, core: 2. Of those that a mesh axis runs over, the one named last changes fastest.
The devices are a block of a 4x4x8 slice.
Arguments:
- x: bfloat16 [16, 2048, 768], P(('rep', 'dp')), parts along dimension 0
- dy: bfloat16 [16, 2048, 768], P(('rep', 'dp')), parts along dimension 0
- w_gate: bfloat16 [2, 768, 1792], replicated
- w_up: bfloat16 [2, 768, 1792], replicated
- w_down: bfloat16 [2, 1792, 768], replicated
- m_w_gate: float32 [2, 768, 1792], replicated
- m_w_up: float32 [2, 768, 1792], replicated
- m_w_down: float32 [2, 1792, 768], replicated
- v_w_gate: float32 [2, 768, 1792], replicated
- v_w_up: float32 [2, 768, 1792], replicated
- v_w_down: float32 [2, 1792, 768], replicated
Outputs:
- output 1: bfloat16 [4, 768, 1792], P('rep'), parts along dimension 0
- output 2: bfloat16 [4, 768, 1792], P('rep'), parts along dimension 0
- output 3: bfloat16 [4, 1792, 768], P('rep'), parts along dimension 0
- output 4: float32 [4, 768, 1792], P('rep'), parts along dimension 0
- output 5: float32 [4, 768, 1792], P('rep'), parts along dimension 0
- output 6: float32 [4, 1792, 768], P('rep'), parts along dimension 0
- output 7: float32 [4, 768, 1792], P('rep'), parts along dimension 0
- output 8: float32 [4, 768, 1792], P('rep'), parts along dimension 0
- output 9: float32 [4, 1792, 768], P('rep'), parts along dimension 0
There are 2 independent parts. The reference program is written for one: setup_inputs(seed, part) draws one part's arguments, and reference() takes and returns one part's arrays. A program takes and returns all parts, laid end to end along the dimension named above; an argument that names none is the same for every part.
All inputs are finite; a program needn't handle non-finite values.
Results may differ from the reference program's by a relative error of at most 0.022.
Values are sent between devices in bfloat16 or wider.
A program may use at most 768 MiB of HBM per device.

```python
import jax
import jax.numpy as jnp
from jax import lax

SEQUENCES = 8
TOKENS = 2048
D = 768
FF = 1792
LAYERS = 2
NAMES = ("w_gate", "w_up", "w_down")
SHAPES = {"w_gate": (LAYERS, D, FF), "w_up": (LAYERS, D, FF), "w_down": (LAYERS, FF, D)}


def bump(key, n, height):
    away = (jnp.arange(n, dtype=jnp.int32) - jax.random.randint(key, (), 0, n, jnp.int32)) % n
    return jnp.where(away < n // 8, height, 1.0)


def together(key, own, strength):
    shared = jax.random.normal(key, own.shape[1:], jnp.float32)
    return (own + strength * shared) * lax.rsqrt(1 + strength * strength)


def setup_inputs(seed: int = 0, part: int = 0) -> dict:
    kx, kdy, ka, kb, kz, kf, kh, kl, *keys = jax.random.split(jax.random.key(seed), 8 + 3 * len(NAMES))
    kx, kdy, ka, kb = (jax.random.fold_in(k, part) for k in (kx, kdy, ka, kb))
    kw, km, kv = (keys[i::3] for i in range(3))
    shape = (SEQUENCES, TOKENS, D)
    much_x, much_dy = jax.random.uniform(kz, (2,), jnp.float32, 0.0, 1.0)
    loud = 2.0 ** jax.random.uniform(jax.random.fold_in(kz, 1), (), jnp.float32, -1.0, 2.0)
    layers = 2.0 ** jax.random.uniform(kl, (LAYERS, 1, 1), jnp.float32, -1.0, 1.0)
    x = together(ka, jax.random.normal(kx, shape, jnp.float32), much_x) * bump(kf, D, 4.0)
    dy = together(kb, jax.random.normal(kdy, shape, jnp.float32), much_dy)
    drawn = {"x": x.astype(jnp.bfloat16), "dy": (loud * dy * (SEQUENCES * TOKENS) ** -0.5).astype(jnp.bfloat16)}
    for key, name in zip(kw, NAMES, strict=True):
        w = jax.random.normal(key, SHAPES[name], jnp.float32) * SHAPES[name][1] ** -0.5
        drawn[name] = (w * {"w_gate": 1.0, "w_up": bump(kh, FF, 4.0), "w_down": layers}[name]).astype(jnp.bfloat16)
    for key, name in zip(km, NAMES, strict=True):
        drawn[f"m_{name}"] = 0.1 * jax.random.normal(key, SHAPES[name], jnp.float32)
    for key, name in zip(kv, NAMES, strict=True):
        drawn[f"v_{name}"] = jax.random.uniform(key, SHAPES[name], jnp.float32, 0.005, 0.015)
    return drawn


def matmul(a, w):
    return jnp.dot(a, w, preferred_element_type=jnp.float32).astype(jnp.bfloat16)


def normed(h):
    wide = h.astype(jnp.float32)
    scale = lax.rsqrt(jnp.mean(wide**2, -1, keepdims=True) + 1e-6)
    return (wide * scale).astype(jnp.bfloat16)


def layer(h, w):
    a = normed(h)
    gate = jnp.dot(a, w["w_gate"], preferred_element_type=jnp.float32)
    up = jnp.dot(a, w["w_up"], preferred_element_type=jnp.float32)
    return h + matmul((jax.nn.silu(gate) * up).astype(jnp.bfloat16), w["w_down"])


def adamw(w, m, v, g):
    m = 0.9 * m + 0.1 * g
    v = 0.95 * v + 0.05 * g * g
    step = m * lax.rsqrt(v + 1e-8) + 0.1 * w
    return (w - 0.02 * step).astype(jnp.bfloat16), m, v


def clipped(gradients, sum_of_squares, count):
    factor = jnp.minimum(1.0, 0.5 * lax.rsqrt(sum_of_squares / count + 1e-30))
    return [g * factor for g in gradients]


def stack(weights, h):
    return lax.scan(lambda h, w: (layer(h, w), None), h, weights)[0]


def reference(x, dy, w_gate, w_up, w_down, m_w_gate, m_w_up, m_w_down, v_w_gate, v_w_up, v_w_down):
    weights = dict(zip(NAMES, (w_gate, w_up, w_down), strict=True))

    def take(so_far, sequence):
        h, by_y = sequence
        _, back = jax.vjp(lambda w: stack(w, h), weights)
        return jax.tree.map(lambda total, term: total + term.astype(jnp.float32), so_far, back(by_y)[0]), None

    none_yet = {name: jnp.zeros(w.shape, jnp.float32) for name, w in weights.items()}
    by_weights, _ = lax.scan(take, none_yet, (x, dy))
    gradients = [by_weights[name].astype(jnp.bfloat16).astype(jnp.float32) for name in NAMES]
    gradients = clipped(gradients, sum(jnp.sum(g * g) for g in gradients), sum(g.size for g in gradients))
    new = [
        adamw(w.astype(jnp.float32), m, v, g)
        for w, m, v, g in zip((w_gate, w_up, w_down), (m_w_gate, m_w_up, m_w_down), (v_w_gate, v_w_up, v_w_down), gradients, strict=True)
    ]
    return tuple(one[which] for which in range(3) for one in new)
```

```python
import functools

import jax
import jax.numpy as jnp
from jax import lax
from jax.experimental import pallas as pl
from jax.experimental.pallas import tpu as pltpu
from jax.sharding import PartitionSpec as P

NAMES = ("w_gate", "w_up", "w_down")
BLOCKS = 8


def matmul(a, w):
    return jnp.dot(a, w, preferred_element_type=jnp.float32).astype(jnp.bfloat16)


def normed(h):
    wide = h.astype(jnp.float32)
    scale = lax.rsqrt(jnp.mean(wide**2, -1, keepdims=True) + 1e-6)
    return (wide * scale).astype(jnp.bfloat16)


def layer(h, w):
    a = normed(h)
    gate = jnp.dot(a, w["w_gate"], preferred_element_type=jnp.float32)
    up = jnp.dot(a, w["w_up"], preferred_element_type=jnp.float32)
    return h + matmul((jax.nn.silu(gate) * up).astype(jnp.bfloat16), w["w_down"])


def adamw_kernel(factor_ref, *refs):
    g, w, m, v = (refs[i : i + 3] for i in (0, 3, 6, 9))
    new_w, new_m, new_v = (refs[len(refs) - 9 :][i : i + 3] for i in (0, 3, 6))
    factor = factor_ref[0]
    for i in range(3):
        grad = g[i][...].astype(jnp.float32) * factor
        mean = 0.9 * m[i][0] + 0.1 * grad
        square = 0.95 * v[i][0] + 0.05 * grad * grad
        wide = w[i][0].astype(jnp.float32)
        new_w[i][0] = (wide - 0.02 * (mean * lax.rsqrt(square + 1e-8) + 0.1 * wide)).astype(jnp.bfloat16)
        new_m[i][0] = mean
        new_v[i][0] = square


def adamw(number, factor, gradients, weights, m, v, so_far):
    whole = [(1, w.shape[1] // BLOCKS, w.shape[2]) for w in weights]
    at_layer = [pl.BlockSpec(s, lambda i: (number, i, 0)) for s in whole]
    alone = [pl.BlockSpec(s[1:], lambda i: (i, 0)) for s in whole]
    carried = [] if so_far is None else list(so_far)
    return pl.pallas_call(
        adamw_kernel,
        grid=(BLOCKS,),
        in_specs=[pl.BlockSpec(memory_space=pltpu.SMEM)] + alone + at_layer * 3 + [pl.BlockSpec(memory_space=pl.ANY)] * len(carried),
        out_specs=at_layer * 3,
        out_shape=[jax.ShapeDtypeStruct(a.shape, a.dtype) for a in (*weights, *m, *v)],
        input_output_aliases={13 + i: i for i in range(len(carried))},
        compiler_params=pltpu.CompilerParams(dimension_semantics=("arbitrary",), vmem_limit_bytes=48 * 2**20),
        cost_estimate=pl.CostEstimate(flops=16 * sum(w.size for w in weights), bytes_accessed=11 * sum(w.size for w in weights), transcendentals=0),
        name=f"adamw_{number}",
    )(factor, *gradients, *weights, *m, *v, *carried)


def solution(mesh):
    def step(x, dy, *arrays):
        weights, m, v = (arrays[i : i + 3] for i in (0, 3, 6))
        layers = weights[0].shape[0]
        h, kept = x[0], []
        for number in range(layers):
            kept.append(h)
            h = layer(h, {name: w[number] for name, w in zip(NAMES, weights, strict=True)})
        by_h, scattered = dy[0], [None] * layers
        before = None
        for number in reversed(range(layers)):
            _, back = jax.vjp(lambda w, h: layer(h, w), {name: w[number] for name, w in zip(NAMES, weights, strict=True)}, kept[number])
            by_w, by_h = back(by_h)
            terms = [by_w[name] for name in NAMES]
            if before is not None:
                terms, _ = lax.optimization_barrier((terms, before))
            before = scattered[number] = [lax.psum_scatter(t, "dp", scatter_dimension=0, tiled=True) for t in terms]
        total = sum(jnp.sum(s.astype(jnp.float32) ** 2) for one in scattered for s in one)
        total = lax.psum(total, "dp")
        count = sum(w.size for w in weights)
        factor = jnp.minimum(1.0, 0.5 * lax.rsqrt(total / count + 1e-30)).reshape(1)
        so_far, before = None, None
        for number in reversed(range(layers)):
            shards = scattered[number]
            if before is not None:
                shards, _ = lax.optimization_barrier((shards, before))
            before = gathered = [lax.all_gather(s, "dp", axis=0, tiled=True) for s in shards]
            so_far = adamw(number, factor, gathered, weights, m, v, so_far)
        return tuple(so_far)

    return jax.shard_map(
        step,
        mesh=mesh,
        in_specs=(P(("rep", "dp"), None, None),) * 2 + (P(None, None, None),) * 9,
        out_specs=(P("rep", None, None),) * 9,
        check_vma=False,
    )
```

```python
import functools

import jax
import jax.numpy as jnp
from jax import lax
from jax.experimental import pallas as pl
from jax.experimental.pallas import tpu as pltpu
from jax.sharding import PartitionSpec as P

CHUNK = 256
TILE = 512
F32, BF16 = jnp.float32, jnp.bfloat16


def dot(a, b, contract):
    return lax.dot_general(a, b, (contract, ((), ())), preferred_element_type=F32)


def scale_of(wide):
    return lax.rsqrt(jnp.mean(wide * wide, -1, keepdims=True) + 1e-6)


def forward_kernel(x_ref, wg_ref, wu_ref, wd_ref, h_ref, hid):
    wide = x_ref[...].astype(F32)
    a = (wide * scale_of(wide)).astype(BF16)
    for at in range(0, hid.shape[1], CHUNK):
        gate = dot(a, wg_ref[0, :, at : at + CHUNK], ((1,), (0,)))
        up = dot(a, wu_ref[0, :, at : at + CHUNK], ((1,), (0,)))
        hid[:, at : at + CHUNK] = (gate * jax.nn.sigmoid(gate) * up).astype(BF16)
    out = dot(hid[...], wd_ref[0], ((1,), (0,))).astype(BF16)
    h_ref[...] = (wide + out.astype(F32)).astype(BF16)


def forward(number, x, wg, wu, wd):
    tokens, d = x.shape
    whole = lambda w: pl.BlockSpec((1, *w.shape[1:]), lambda i: (number, 0, 0))
    rows = pl.BlockSpec((min(TILE, tokens), d), lambda i: (i, 0))
    return pl.pallas_call(
        forward_kernel,
        grid=(tokens // min(TILE, tokens),),
        in_specs=[rows, whole(wg), whole(wu), whole(wd)],
        out_specs=rows,
        out_shape=jax.ShapeDtypeStruct(x.shape, BF16),
        scratch_shapes=[pltpu.VMEM((min(TILE, tokens), wg.shape[2]), BF16)],
        compiler_params=pltpu.CompilerParams(dimension_semantics=("arbitrary",), vmem_limit_bytes=48 * 2**20),
        name="forward",
    )(x, wg, wu, wd)


def train_kernel(
    n, layers, per_layer, comm,
    x_hbm, h_hbm, dy_hbm, wg_hbm, wu_hbm, wd_hbm,
    sum_hbm, norm_hbm,
    h, dy, a, a_t, da, wgu, wd, hid, dgu, g,
    recv_p, recv_1, recv_2, wide_sum, send_1, send_2, red, squares, all_squares,
    load_sem, w_sem, send_sem, recv_sem, keep_sem, norm_send, norm_recv,
):
    tokens, d = h.shape
    tile = min(TILE, tokens)
    tiles = tokens // tile
    chunks = layers * per_layer
    me = lax.axis_index("dp")
    chip, core = me // 2, me % 2
    chips = n // 2
    right = lax.rem(chip + 1, chips) * 2 + core
    left = lax.rem(chip + chips - 1, chips) * 2 + core
    partner = chip * 2 + 1 - core
    half = g.shape[1] // 2
    shard = half // chips
    part = shard // 2
    mine = pl.multiple_of(core * half, 16)
    theirs = pl.multiple_of((1 - core) * half, 16)

    def at_shard(q):
        return pl.multiple_of(lax.rem(chip + q, chips) * shard, 16)

    def remote(src, dst, c, k, to):
        return pltpu.make_async_remote_copy(
            src_ref=src, dst_ref=dst, send_sem=send_sem.at[c, k], recv_sem=recv_sem.at[c, k],
            device_id={"dp": to}, device_id_type=pl.DeviceIdType.MESH,
        )

    def load_weights(it, slot):
        layer, j = layers - 1 - it // per_layer, lax.rem(it, per_layer)
        columns = pl.ds(pl.multiple_of(j * CHUNK, CHUNK), CHUNK)
        return (
            pltpu.make_async_copy(wg_hbm.at[layer, :, columns], wgu.at[slot, :, pl.ds(0, CHUNK)], w_sem.at[slot, 0]),
            pltpu.make_async_copy(wu_hbm.at[layer, :, columns], wgu.at[slot, :, pl.ds(CHUNK, CHUNK)], w_sem.at[slot, 1]),
            pltpu.make_async_copy(wd_hbm.at[layer, columns, :], wd.at[slot], w_sem.at[slot, 2]),
        )

    def pair(c, slot):
        return remote(g.at[slot, pl.ds(theirs, half)], recv_p.at[c], c, 0, partner)

    def first(c, slot, k):
        return remote(send_1.at[slot, k], recv_1.at[c, k], c, 1 + k, (right, left)[k])

    def second(c, slot, k):
        return remote(send_2.at[slot, k], recv_2.at[c, k], c, 3 + k, (right, left)[k])

    def spread(c, slot, k):
        rows = pl.ds(mine + at_shard(0), shard)
        return remote(red.at[slot], sum_hbm.at[c, rows], c, 5 + k, (right, left)[k])

    def keep(c, slot):
        return pltpu.make_async_copy(red.at[slot], sum_hbm.at[c, pl.ds(mine + at_shard(0), shard)], keep_sem.at[c])

    def forward_on(c, k):
        rows = pl.ds(mine + at_shard((chips - 1, 1)[k]) + k * part, part)
        return remote(sum_hbm.at[c, rows], sum_hbm.at[c, rows], c, 7 + k, (right, left)[k])

    def pair_back(c):
        rows = pl.ds(mine, half)
        return remote(sum_hbm.at[c, rows], sum_hbm.at[c, rows], c, 9, partner)

    others = [lax.rem(me + k, n) for k in range(1, n)]
    if comm:
        barrier = pltpu.get_barrier_semaphore()
        for other in others:
            pl.semaphore_signal(barrier, inc=1, device_id={"dp": other}, device_id_type=pl.DeviceIdType.MESH)

    loads = [pltpu.make_async_copy(src, dst, load_sem.at[i]) for i, (src, dst) in enumerate([(h_hbm, h), (dy_hbm, dy)])]
    for load in loads:
        load.start()
    for load in load_weights(0, 0):
        load.start()
    squares[...] = jnp.zeros_like(squares)
    if comm:
        pl.semaphore_wait(barrier, n - 1)
    loads[0].wait()

    def prepare():
        def body(t, _):
            rows = pl.ds(pl.multiple_of(t * tile, tile), tile)
            wide = h[rows, :].astype(F32)
            normed = (wide * scale_of(wide)).astype(BF16)
            a[rows, :] = normed
            a_t[:, rows] = normed.T
            return 0

        lax.fori_loop(0, tiles, body, 0)

    prepare()
    da[...] = jnp.zeros_like(da)
    loads[1].wait()

    def next_layer():
        def body(t, _):
            rows = pl.ds(pl.multiple_of(t * tile, tile), tile)
            wide, by_a = h[rows, :].astype(F32), da[rows, :].astype(BF16).astype(F32)
            scale = scale_of(wide)
            inner = jnp.sum(by_a * wide, -1, keepdims=True)
            by_h = (by_a * scale - wide * (scale * scale * scale * inner * (1.0 / d))).astype(BF16)
            dy[rows, :] = (dy[rows, :].astype(F32) + by_h.astype(F32)).astype(BF16)
            return 0

        lax.fori_loop(0, tiles, body, 0)
        load = pltpu.make_async_copy(x_hbm, h, load_sem.at[0])
        load.start()
        load.wait()
        prepare()

    def compute(it):
        slot = lax.rem(it, 2)
        for load in load_weights(it, slot):
            load.wait()

        @pl.when(it + 1 < chunks)
        def _():
            for load in load_weights(it + 1, 1 - slot):
                load.start()

        def body(t, _):
            rows = pl.ds(pl.multiple_of(t * tile, tile), tile)
            both = dot(a[rows, :], wgu[slot], ((1,), (0,)))
            by_hid = dot(dy[rows, :], wd[slot], ((1,), (1,))).astype(BF16).astype(F32)
            gate, up = both[:, :CHUNK], both[:, CHUNK:]
            sig = jax.nn.sigmoid(gate)
            act = gate * sig
            hid[rows, :] = (act * up).astype(BF16)
            dgu[rows, :CHUNK] = (by_hid * up * (sig + act * (1.0 - sig))).astype(BF16)
            dgu[rows, CHUNK:] = (by_hid * act).astype(BF16)

            @pl.when(it < (layers - 1) * per_layer)
            def _():
                da[rows, :] += dot(dgu[rows, :], wgu[slot], ((1,), (1,)))

            return 0

        lax.fori_loop(0, tiles, body, 0)
        by_wd = dot(hid[...], dy[...], ((0,), (0,))).astype(BF16)
        for k in range(d // CHUNK):
            g[slot, 2 * d + k * CHUNK : 2 * d + (k + 1) * CHUNK, :] = by_wd[:, k * CHUNK : (k + 1) * CHUNK]
        by_wgu = dot(a_t[...], dgu[...], ((1,), (0,))).astype(BF16)
        g[slot, :d, :] = by_wgu[:, :CHUNK]
        g[slot, d : 2 * d, :] = by_wgu[:, CHUNK:]

    def within(c, act):
        pl.when((c >= 0) & (c < chunks))(act)

    def serve(it):
        def last():
            c = it - 6
            pair_back(c).wait()

        within(it - 6, last)

        def five():
            c = it - 5
            for k in range(2):
                forward_on(c, k).wait()
            pair_back(c).start()

        within(it - 5, five)

        def four():
            c = it - 4
            keep(c, lax.rem(c, 2)).wait()
            for k in range(2):
                spread(c, lax.rem(c, 2), k).wait()
            for k in range(2):
                forward_on(c, k).start()

        within(it - 4, four)

        def three():
            c = it - 3
            for k in range(2):
                second(c, lax.rem(c, 2), k).wait()
            total = wide_sum[lax.rem(c, 3), pl.ds(at_shard(0), shard), :]
            total = (total + recv_2[c, 0].astype(F32) + recv_2[c, 1].astype(F32)).astype(BF16)
            red[lax.rem(c, 2)] = total
            spread(c, lax.rem(c, 2), 0).start()
            spread(c, lax.rem(c, 2), 1).start()
            keep(c, lax.rem(c, 2)).start()
            total = total.astype(F32)
            squares[...] += jnp.sum((total * total).reshape(shard // 8, 8, CHUNK), 0)

        within(it - 3, three)

        def two():
            c = it - 2
            for k in range(2):
                first(c, lax.rem(c, 2), k).wait()
            for k, q in enumerate((1, chips - 1)):
                rows = wide_sum[lax.rem(c, 3), pl.ds(at_shard(q), shard), :]
                extra = recv_1[c, k].astype(F32)
                send_2[lax.rem(c, 2), k, k * part : (k + 1) * part] = (rows[k * part : (k + 1) * part] + extra).astype(BF16)
                send_2[lax.rem(c, 2), k, (1 - k) * part : (2 - k) * part] = rows[(1 - k) * part : (2 - k) * part].astype(BF16)
                second(c, lax.rem(c, 2), k).start()

        within(it - 2, two)

        def one():
            c = it - 1
            pair(c, lax.rem(c, 2)).wait()
            wide_sum[lax.rem(c, 3)] = g[lax.rem(c, 2), pl.ds(mine, half), :].astype(F32) + recv_p[c].astype(F32)
            for k in range(2):
                send_1[lax.rem(c, 2), k] = wide_sum[lax.rem(c, 3), pl.ds(at_shard(2) + k * part, part), :].astype(BF16)
                first(c, lax.rem(c, 2), k).start()

        within(it - 1, one)

    def step(it, _):
        if comm:
            serve(it)
        pl.when(it == (layers - 1) * per_layer)(next_layer)
        pl.when(it < chunks)(lambda: compute(it))
        if comm:
            pl.when(it < chunks)(lambda: pair(it, lax.rem(it, 2)).start())
        return 0

    lax.fori_loop(0, chunks + 7 if comm else chunks, step, 0)

    if comm:
        all_squares[pl.ds(me, 1)] = squares[...][None]
        sends = [
            pltpu.make_async_remote_copy(
                src_ref=squares, dst_ref=all_squares.at[me], send_sem=norm_send.at[k], recv_sem=norm_recv.at[k],
                device_id={"dp": other}, device_id_type=pl.DeviceIdType.MESH,
            )
            for k, other in enumerate(others)
        ]
        for send in sends:
            send.start()
        for send in sends:
            send.wait()
        total = all_squares[0]
        for k in range(1, n):
            total += all_squares[k]
        norm_hbm[...] = total
    else:
        norm_hbm[...] = squares[...]
        pltpu.sync_copy(g.at[0], sum_hbm.at[0])


def train(n, x, h, dy, wg, wu, wd, comm=True):
    tokens, d = x.shape
    layers, _, ff = wg.shape
    per_layer = ff // CHUNK
    chunks, rows = layers * per_layer, 3 * d
    half = rows // 2
    shard = half // (n // 2)
    part = shard // 2
    hbm = pl.BlockSpec(memory_space=pl.ANY)
    vmem = pltpu.VMEM
    dma = pltpu.SemaphoreType.DMA
    return pl.pallas_call(
        functools.partial(train_kernel, n, layers, per_layer, comm),
        in_specs=[hbm] * 6,
        out_specs=[hbm, pl.BlockSpec(memory_space=pltpu.VMEM)],
        out_shape=[jax.ShapeDtypeStruct((chunks, rows, CHUNK), BF16), jax.ShapeDtypeStruct((8, CHUNK), F32)],
        scratch_shapes=[
            vmem((tokens, d), BF16), vmem((tokens, d), BF16), vmem((tokens, d), BF16), vmem((d, tokens), BF16), vmem((tokens, d), F32),
            vmem((2, d, 2 * CHUNK), BF16), vmem((2, CHUNK, d), BF16), vmem((tokens, CHUNK), BF16), vmem((tokens, 2 * CHUNK), BF16),
            vmem((2, rows, CHUNK), BF16),
            vmem((chunks, half, CHUNK), BF16), vmem((chunks, 2, part, CHUNK), BF16), vmem((chunks, 2, shard, CHUNK), BF16),
            vmem((3, half, CHUNK), F32), vmem((2, 2, part, CHUNK), BF16), vmem((2, 2, shard, CHUNK), BF16), vmem((2, shard, CHUNK), BF16),
            vmem((8, CHUNK), F32), vmem((n, 8, CHUNK), F32),
            dma((2,)), dma((2, 3)), dma((chunks, 10)), dma((chunks, 10)), dma((chunks,)), dma((n - 1,)), dma((n - 1,)),
        ],
        compiler_params=pltpu.CompilerParams(collective_id=0 if comm else None, has_side_effects=True, vmem_limit_bytes=63 * 2**20),
        cost_estimate=pl.CostEstimate(flops=14 * tokens * d * ff * layers, bytes_accessed=60 * 2**20, transcendentals=0),
        name="train",
    )(x, h, dy, wg, wu, wd)


def adamw_kernel(count, squares_ref, g_ref, *refs):
    w, m, v, new_w, new_m, new_v = (refs[i : i + 3] for i in range(0, 18, 3))
    total = jnp.sum(squares_ref[...], (0, 1), keepdims=True)
    factor = jnp.minimum(1.0, 0.5 * lax.rsqrt(total / count + 1e-30))
    d = w[0].shape[1]
    for i in range(3):
        if i < 2:
            grad = g_ref[0, i * d : (i + 1) * d, :]
        else:
            grad = jnp.concatenate([g_ref[0, 2 * d + k : 2 * d + k + CHUNK, :] for k in range(0, d, CHUNK)], 1)
        grad = grad.astype(F32) * factor
        mean = 0.9 * m[i][0] + 0.1 * grad
        square = 0.95 * v[i][0] + 0.05 * grad * grad
        wide = w[i][0].astype(F32)
        new_w[i][0] = (wide - 0.02 * (mean * lax.rsqrt(square + 1e-8) + 0.1 * wide)).astype(BF16)
        new_m[i][0] = mean
        new_v[i][0] = square


def adamw(squares, g, weights, m, v):
    layers, d, ff = weights[0].shape
    per_layer = ff // CHUNK
    across = pl.BlockSpec((1, d, CHUNK), lambda i: (layers - 1 - i // per_layer, 0, i % per_layer))
    down = pl.BlockSpec((1, CHUNK, d), lambda i: (layers - 1 - i // per_layer, i % per_layer, 0))
    each = [across, across, down] * 3
    count = sum(w.size for w in weights)
    return pl.pallas_call(
        functools.partial(adamw_kernel, count),
        grid=(layers * per_layer,),
        in_specs=[pl.BlockSpec((8, CHUNK), lambda i: (0, 0)), pl.BlockSpec((1, 3 * d, CHUNK), lambda i: (i, 0, 0))] + each,
        out_specs=each,
        out_shape=[jax.ShapeDtypeStruct(t.shape, t.dtype) for t in (*weights, *m, *v)],
        compiler_params=pltpu.CompilerParams(dimension_semantics=("arbitrary",), vmem_limit_bytes=48 * 2**20),
        cost_estimate=pl.CostEstimate(flops=16 * count, bytes_accessed=22 * count, transcendentals=0),
        name="adamw",
    )(squares, g, *weights, *m, *v)


def solution(mesh):
    n = mesh.shape["dp"]

    def step(x, dy, *arrays):
        weights, m, v = (arrays[i : i + 3] for i in (0, 3, 6))
        h = forward(0, x[0], *weights)
        g, squares = train(n, x[0], h, dy[0], *weights)
        return tuple(adamw(squares, g, weights, m, v))

    return jax.shard_map(
        step,
        mesh=mesh,
        in_specs=(P(("rep", "dp"), None, None),) * 2 + (P(None, None, None),) * 9,
        out_specs=(P("rep", None, None),) * 9,
        check_vma=False,
    )
```

```python
import functools

import jax
import jax.numpy as jnp
from jax import lax
from jax.experimental import pallas as pl
from jax.experimental.pallas import tpu as pltpu
from jax.sharding import PartitionSpec as P

CHUNK = 256
TILE = 512
GATHERED = 6
F32, BF16 = jnp.float32, jnp.bfloat16


def dot(a, b, contract):
    return lax.dot_general(a, b, (contract, ((), ())), preferred_element_type=F32)


def scale_of(wide):
    return lax.rsqrt(jnp.mean(wide * wide, -1, keepdims=True) + 1e-6)


def forward_kernel(x_ref, wg_ref, wu_ref, wd_ref, h_ref, hid):
    wide = x_ref[...].astype(F32)
    a = (wide * scale_of(wide)).astype(BF16)
    for at in range(0, hid.shape[1], CHUNK):
        gate = dot(a, wg_ref[0, :, at : at + CHUNK], ((1,), (0,)))
        up = dot(a, wu_ref[0, :, at : at + CHUNK], ((1,), (0,)))
        hid[:, at : at + CHUNK] = (gate * (0.5 * jnp.tanh(0.5 * gate) + 0.5) * up).astype(BF16)
    out = dot(hid[...], wd_ref[0], ((1,), (0,))).astype(BF16)
    h_ref[...] = (wide + out.astype(F32)).astype(BF16)


def forward(number, x, wg, wu, wd):
    tokens, d = x.shape
    whole = lambda w: pl.BlockSpec((1, *w.shape[1:]), lambda i: (number, 0, 0))
    rows = pl.BlockSpec((min(TILE, tokens), d), lambda i: (i, 0))
    return pl.pallas_call(
        forward_kernel,
        grid=(tokens // min(TILE, tokens),),
        in_specs=[rows, whole(wg), whole(wu), whole(wd)],
        out_specs=rows,
        out_shape=jax.ShapeDtypeStruct(x.shape, BF16),
        scratch_shapes=[pltpu.VMEM((min(TILE, tokens), wg.shape[2]), BF16)],
        compiler_params=pltpu.CompilerParams(dimension_semantics=("arbitrary",), vmem_limit_bytes=48 * 2**20),
        name="forward",
    )(x, wg, wu, wd)


def train_kernel(
    n, layers, per_layer, gathered, comm,
    x_hbm, h_hbm, dy_hbm, wg_hbm, wu_hbm, wd_hbm,
    sum_hbm, low_hbm, high_hbm, norm_hbm,
    h, dy, a, a_t, da, wgu, wd, hid, dgu, g,
    recv_p, recv_1, recv_2, wide_sum, send_1, send_2, red, squares, all_squares,
    load_sem, w_sem, send_sem, recv_sem, keep_sem, norm_send, norm_recv,
):
    tokens, d = h.shape
    tile = min(TILE, tokens)
    tiles = tokens // tile
    chunks = layers * per_layer
    lows = low_hbm.shape[0]
    me = lax.axis_index("dp")
    chip, core = me // 2, me % 2
    chips = n // 2
    right = lax.rem(chip + 1, chips) * 2 + core
    left = lax.rem(chip + chips - 1, chips) * 2 + core
    partner = chip * 2 + 1 - core
    half = g.shape[1] // 2
    shard = half // chips
    part = shard // 2
    mine = pl.multiple_of(core * half, 16)
    theirs = pl.multiple_of((1 - core) * half, 16)

    def at_shard(q):
        return pl.multiple_of(lax.rem(chip + q, chips) * shard, 16)

    def remote(src, dst, c, k, to):
        return pltpu.make_async_remote_copy(
            src_ref=src, dst_ref=dst, send_sem=send_sem.at[c, k], recv_sem=recv_sem.at[c, k],
            device_id={"dp": to}, device_id_type=pl.DeviceIdType.MESH,
        )

    def load_weights(it, slot):
        layer, j = layers - 1 - it // per_layer, lax.rem(it, per_layer)
        columns = pl.ds(pl.multiple_of(j * CHUNK, CHUNK), CHUNK)
        return (
            pltpu.make_async_copy(wg_hbm.at[layer, :, columns], wgu.at[slot, :, pl.ds(0, CHUNK)], w_sem.at[slot, 0]),
            pltpu.make_async_copy(wu_hbm.at[layer, :, columns], wgu.at[slot, :, pl.ds(CHUNK, CHUNK)], w_sem.at[slot, 1]),
            pltpu.make_async_copy(wd_hbm.at[layer, columns, :], wd.at[slot], w_sem.at[slot, 2]),
        )

    def pair(c, slot):
        return remote(g.at[slot, pl.ds(theirs, half)], recv_p.at[c], c, 0, partner)

    def first(c, slot, k):
        return remote(send_1.at[slot, k], recv_1.at[c, k], c, 1 + k, (right, left)[k])

    def second(c, slot, k):
        return remote(send_2.at[slot, k], recv_2.at[c, k], c, 3 + k, (right, left)[k])

    def spread(c, slot, k):
        rows = pl.ds(mine + at_shard(0), shard)
        return remote(red.at[slot], sum_hbm.at[c, rows], c, 5 + k, (right, left)[k])

    def keep(c, slot, which):
        to = (sum_hbm.at[c, pl.ds(mine + at_shard(0), shard)], low_hbm.at[c - gathered], high_hbm.at[c - gathered - lows])[which]
        return pltpu.make_async_copy(red.at[slot], to, keep_sem.at[c])

    def forward_on(c, k):
        rows = pl.ds(mine + at_shard((chips - 1, 1)[k]) + k * part, part)
        return remote(sum_hbm.at[c, rows], sum_hbm.at[c, rows], c, 7 + k, (right, left)[k])

    def pair_back(c):
        rows = pl.ds(mine, half)
        return remote(sum_hbm.at[c, rows], sum_hbm.at[c, rows], c, 9, partner)

    others = [lax.rem(me + k, n) for k in range(1, n)]
    if comm:
        barrier = pltpu.get_barrier_semaphore()
        for other in others:
            pl.semaphore_signal(barrier, inc=1, device_id={"dp": other}, device_id_type=pl.DeviceIdType.MESH)

    loads = [pltpu.make_async_copy(src, dst, load_sem.at[i]) for i, (src, dst) in enumerate([(h_hbm, h), (dy_hbm, dy)])]
    for load in loads:
        load.start()
    for load in load_weights(0, 0):
        load.start()
    squares[...] = jnp.zeros_like(squares)
    if comm:
        pl.semaphore_wait(barrier, n - 1)
    loads[0].wait()

    def prepare():
        def body(t, _):
            rows = pl.ds(pl.multiple_of(t * tile, tile), tile)
            wide = h[rows, :].astype(F32)
            normed = (wide * scale_of(wide)).astype(BF16)
            a[rows, :] = normed
            a_t[:, rows] = normed.T
            return 0

        lax.fori_loop(0, tiles, body, 0)

    prepare()
    da[...] = jnp.zeros_like(da)
    loads[1].wait()

    def next_layer():
        def body(t, _):
            rows = pl.ds(pl.multiple_of(t * tile, tile), tile)
            wide, by_a = h[rows, :].astype(F32), da[rows, :].astype(BF16).astype(F32)
            scale = scale_of(wide)
            inner = jnp.sum(by_a * wide, -1, keepdims=True)
            by_h = (by_a * scale - wide * (scale * scale * scale * inner * (1.0 / d))).astype(BF16)
            dy[rows, :] = (dy[rows, :].astype(F32) + by_h.astype(F32)).astype(BF16)
            return 0

        lax.fori_loop(0, tiles, body, 0)
        load = pltpu.make_async_copy(x_hbm, h, load_sem.at[0])
        load.start()
        load.wait()
        prepare()

    def compute_hidden(it):
        slot = lax.rem(it, 2)
        for load in load_weights(it, slot):
            load.wait()

        @pl.when(it + 1 < chunks)
        def _():
            for load in load_weights(it + 1, 1 - slot):
                load.start()

        def products(t):
            rows = slice(t * tile, (t + 1) * tile)
            return dot(a[rows, :], wgu[slot], ((1,), (0,))), dot(dy[rows, :], wd[slot], ((1,), (1,)))

        ready = products(0)
        for t in range(tiles):
            (both, by_hid), rows = ready, slice(t * tile, (t + 1) * tile)
            if t + 1 < tiles:
                ready = products(t + 1)
            by_hid = by_hid.astype(BF16).astype(F32)
            gate, up = both[:, :CHUNK], both[:, CHUNK:]
            sig = 0.5 * jnp.tanh(0.5 * gate) + 0.5
            act = gate * sig
            hid[rows, :] = (act * up).astype(BF16)
            dgu[rows, :CHUNK] = (by_hid * up * (sig + act * (1.0 - sig))).astype(BF16)
            dgu[rows, CHUNK:] = (by_hid * act).astype(BF16)

        @pl.when(it < (layers - 1) * per_layer)
        def _():
            def body(t, _):
                rows = pl.ds(pl.multiple_of(t * tile, tile), tile)
                da[rows, :] += dot(dgu[rows, :], wgu[slot], ((1,), (1,)))
                return 0

            lax.fori_loop(0, tiles, body, 0)

    def compute_weights(it):
        slot = lax.rem(it, 2)
        by_wd = dot(hid[...], dy[...], ((0,), (0,))).astype(BF16)
        for k in range(d // CHUNK):
            g[slot, 2 * d + k * CHUNK : 2 * d + (k + 1) * CHUNK, :] = by_wd[:, k * CHUNK : (k + 1) * CHUNK]
        by_wgu = dot(a_t[...], dgu[...], ((1,), (0,))).astype(BF16)
        g[slot, :d, :] = by_wgu[:, :CHUNK]
        g[slot, d : 2 * d, :] = by_wgu[:, CHUNK:]

    def among(c, first_chunk, end, act):
        pl.when((c >= first_chunk) & (c < end))(lambda: act(c, lax.rem(c, 2)))

    def summed(c, slot):
        pair(c, slot).wait()
        wide_sum[lax.rem(c, 3)] = g[slot, pl.ds(mine, half), :].astype(F32) + recv_p[c].astype(F32)
        for k in range(2):
            send_1[slot, k] = wide_sum[lax.rem(c, 3), pl.ds(at_shard(2) + k * part, part), :].astype(BF16)
            first(c, slot, k).start()

    def passed_on(c, slot):
        for k in range(2):
            first(c, slot, k).wait()
        for k, q in enumerate((1, chips - 1)):
            rows = wide_sum[lax.rem(c, 3), pl.ds(at_shard(q), shard), :]
            extra = recv_1[c, k].astype(F32)
            send_2[slot, k, k * part : (k + 1) * part] = (rows[k * part : (k + 1) * part] + extra).astype(BF16)
            send_2[slot, k, (1 - k) * part : (2 - k) * part] = rows[(1 - k) * part : (2 - k) * part].astype(BF16)
            second(c, slot, k).start()

    def finished(c, slot):
        for k in range(2):
            second(c, slot, k).wait()
        total = wide_sum[lax.rem(c, 3), pl.ds(at_shard(0), shard), :]
        total = (total + recv_2[c, 0].astype(F32) + recv_2[c, 1].astype(F32)).astype(BF16)
        red[slot] = total

        @pl.when(c < gathered)
        def _():
            spread(c, slot, 0).start()
            spread(c, slot, 1).start()

        kept(c, lambda which: keep(c, slot, which).start())
        total = total.astype(F32)
        squares[...] += jnp.sum((total * total).reshape(shard // 8, 8, CHUNK), 0)

    def kept(c, act):
        pl.when(c < gathered)(lambda: act(0))
        pl.when((c >= gathered) & (c < gathered + lows))(lambda: act(1))
        pl.when(c >= gathered + lows)(lambda: act(2))

    def spread_on(c, slot):
        kept(c, lambda which: keep(c, slot, which).wait())

        @pl.when(c < gathered)
        def _():
            for k in range(2):
                spread(c, slot, k).wait()
            for k in range(2):
                forward_on(c, k).start()

    def returned(c, slot):
        for k in range(2):
            forward_on(c, k).wait()
        pair_back(c).start()

    def serve_start(it):
        among(it - 3, 0, chunks, passed_on)
        among(it - 6, 0, chunks, spread_on)

    def serve_middle(it):
        among(it - 4, 0, chunks, finished)
        among(it - 1, 0, chunks, summed)
        among(it - 7, 0, gathered, returned)
        among(it - 8, 0, gathered, lambda c, slot: pair_back(c).wait())

    def step(it, _):
        if comm:
            serve_start(it)
        pl.when(it == (layers - 1) * per_layer)(next_layer)
        pl.when(it < chunks)(lambda: compute_hidden(it))
        if comm:
            serve_middle(it)
        pl.when(it < chunks)(lambda: compute_weights(it))
        if comm:
            pl.when(it < chunks)(lambda: pair(it, lax.rem(it, 2)).start())
        return 0

    lax.fori_loop(0, max(chunks + 7, gathered + 9) if comm else chunks, step, 0)

    if comm:
        all_squares[pl.ds(me, 1)] = squares[...][None]
        sends = [
            pltpu.make_async_remote_copy(
                src_ref=squares, dst_ref=all_squares.at[me], send_sem=norm_send.at[k], recv_sem=norm_recv.at[k],
                device_id={"dp": other}, device_id_type=pl.DeviceIdType.MESH,
            )
            for k, other in enumerate(others)
        ]
        for send in sends:
            send.start()
        for send in sends:
            send.wait()
        total = all_squares[0]
        for k in range(1, n):
            total += all_squares[k]
        norm_hbm[...] = total
    else:
        norm_hbm[...] = squares[...]
        pltpu.sync_copy(g.at[0], sum_hbm.at[0])


def train(n, x, h, dy, wg, wu, wd, gathered, comm=True):
    tokens, d = x.shape
    layers, _, ff = wg.shape
    per_layer = ff // CHUNK
    chunks, rows = layers * per_layer, 3 * d
    half = rows // 2
    shard = half // (n // 2)
    part = shard // 2
    lows = (chunks - gathered + 1) // 2
    hbm = pl.BlockSpec(memory_space=pl.ANY)
    vmem = pltpu.VMEM
    dma = pltpu.SemaphoreType.DMA
    return pl.pallas_call(
        functools.partial(train_kernel, n, layers, per_layer, gathered, comm),
        in_specs=[hbm] * 6,
        out_specs=[hbm, hbm, hbm, pl.BlockSpec(memory_space=pltpu.VMEM)],
        out_shape=[jax.ShapeDtypeStruct((k, r, CHUNK), BF16) for k, r in ((gathered, rows), (lows, shard), (chunks - gathered - lows, shard))]
        + [jax.ShapeDtypeStruct((8, CHUNK), F32)],
        scratch_shapes=[
            vmem((tokens, d), BF16), vmem((tokens, d), BF16), vmem((tokens, d), BF16), vmem((d, tokens), BF16), vmem((tokens, d), F32),
            vmem((2, d, 2 * CHUNK), BF16), vmem((2, CHUNK, d), BF16), vmem((tokens, CHUNK), BF16), vmem((tokens, 2 * CHUNK), BF16),
            vmem((2, rows, CHUNK), BF16),
            vmem((chunks, half, CHUNK), BF16), vmem((chunks, 2, part, CHUNK), BF16), vmem((chunks, 2, shard, CHUNK), BF16),
            vmem((3, half, CHUNK), F32), vmem((2, 2, part, CHUNK), BF16), vmem((2, 2, shard, CHUNK), BF16), vmem((2, shard, CHUNK), BF16),
            vmem((8, CHUNK), F32), vmem((n, 8, CHUNK), F32),
            dma((2,)), dma((2, 3)), dma((chunks, 10)), dma((chunks, 10)), dma((chunks,)), dma((n - 1,)), dma((n - 1,)),
        ],
        compiler_params=pltpu.CompilerParams(collective_id=0 if comm else None, has_side_effects=True, vmem_limit_bytes=63 * 2**20),
        cost_estimate=pl.CostEstimate(flops=14 * tokens * d * ff * layers, bytes_accessed=60 * 2**20, transcendentals=0),
        name="train",
    )(x, h, dy, wg, wu, wd)


def adamw_kernel(count, pieces, squares_ref, *refs):
    w, m, v = (refs[pieces + i : pieces + i + 3] for i in (0, 3, 6))
    rest = refs[pieces + 9 :]
    if pieces == 1:
        g, rest = refs[0].at[0], rest[-9:]
    else:
        g, rest = rest[-1], rest[-10:-1]
        me = lax.axis_index("dp")
        chips, shard = pieces // 2, refs[0].shape[1]
        for i in range(pieces):
            core = (me + i // chips) % 2
            at = core * (chips * shard) + lax.rem(me // 2 + (0, chips - 1, 1, 2)[i % chips], chips) * shard
            g[pl.ds(pl.multiple_of(at, 16), shard), :] = refs[i][0]
    new_w, new_m, new_v = rest[:3], rest[3:6], rest[6:]
    total = jnp.sum(squares_ref[...], (0, 1), keepdims=True)
    factor = jnp.minimum(1.0, 0.5 * lax.rsqrt(total / count + 1e-30))
    d = w[0].shape[1]
    for i in range(3):
        if i < 2:
            grad = g[i * d : (i + 1) * d, :]
        else:
            grad = jnp.concatenate([g[2 * d + k : 2 * d + k + CHUNK, :] for k in range(0, d, CHUNK)], 1)
        grad = grad.astype(F32) * factor
        mean = 0.9 * m[i][0] + 0.1 * grad
        square = 0.95 * v[i][0] + 0.05 * grad * grad
        wide = w[i][0].astype(F32)
        new_w[i][0] = (wide - 0.02 * (mean * lax.rsqrt(square + 1e-8) + 0.1 * wide)).astype(BF16)
        new_m[i][0] = mean
        new_v[i][0] = square


def adamw(start, end, squares, gradients, weights, m, v, so_far):
    layers, d, ff = weights[0].shape
    per_layer = ff // CHUNK
    chunks, pieces = end - start, len(gradients)
    skip = start if pieces == 1 else 0
    layer = lambda i: layers - 1 - (start + i) // per_layer
    across = pl.BlockSpec((1, d, CHUNK), lambda i: (layer(i), 0, (start + i) % per_layer))
    down = pl.BlockSpec((1, CHUNK, d), lambda i: (layer(i), (start + i) % per_layer, 0))
    each = [across, across, down] * 3
    count = sum(w.size for w in weights)
    carried = list(so_far or [])
    return pl.pallas_call(
        functools.partial(adamw_kernel, count, pieces),
        grid=(chunks,),
        in_specs=[pl.BlockSpec((8, CHUNK), lambda i: (0, 0))]
        + [pl.BlockSpec((1, *g.shape[1:]), lambda i: (skip + i, 0, 0)) for g in gradients]
        + each
        + [pl.BlockSpec(memory_space=pl.ANY)] * len(carried),
        out_specs=each,
        out_shape=[jax.ShapeDtypeStruct(t.shape, t.dtype) for t in (*weights, *m, *v)],
        scratch_shapes=[] if pieces == 1 else [pltpu.VMEM((3 * d, CHUNK), BF16)],
        input_output_aliases={10 + pieces + i: i for i in range(len(carried))},
        compiler_params=pltpu.CompilerParams(dimension_semantics=("arbitrary",), vmem_limit_bytes=62 * 2**20),
        cost_estimate=pl.CostEstimate(flops=chunks * FLOPS_OF_A_CHUNK, bytes_accessed=chunks * 66 * d * CHUNK, transcendentals=0),
        name=f"adamw_{start}",
    )(squares, *gradients, *weights, *m, *v, *carried)


FLOPS_OF_A_CHUNK = 10**10


def solution(mesh):
    n = mesh.shape["dp"]
    chips = n // 2
    right = [(2 * c + k, (2 * c + 2) % n + k) for c in range(chips) for k in range(2)]
    left = [(to, source) for source, to in right]
    pairs = [(i, i ^ 1) for i in range(n)]

    def go(t, way):
        return lax.ppermute(t, "dp", way)

    def step(x, dy, *arrays):
        weights, m, v = (arrays[i : i + 3] for i in (0, 3, 6))
        h = forward(0, x[0], *weights)
        g, low, high, squares = train(n, x[0], h, dy[0], *weights, GATHERED)
        take = lambda first, end, parts, so_far: adamw(first, end, squares, parts, weights, m, v, so_far)
        lows = [low, go(low, right), go(low, left)]
        highs = [high, go(high, right), go(high, left)]
        new = take(0, GATHERED // 2, [g], None)
        lows, new = lax.optimization_barrier((lows, new))
        lows.append(go(lows[1], right))
        new = take(GATHERED // 2, GATHERED, [g], new)
        lows, highs, new = lax.optimization_barrier((lows, highs, new))
        highs.append(go(highs[2], left))
        end = GATHERED + low.shape[0]
        new = take(GATHERED, end, lows + [go(t, pairs) for t in lows], new)
        highs, new = lax.optimization_barrier((highs, new))
        return tuple(take(end, end + high.shape[0], highs + [go(t, pairs) for t in highs], new))

    return jax.shard_map(
        step,
        mesh=mesh,
        in_specs=(P(("rep", "dp"), None, None),) * 2 + (P(None, None, None),) * 9,
        out_specs=(P("rep", None, None),) * 9,
        check_vma=False,
    )
```

```python
import functools

import jax
import jax.numpy as jnp
from jax import lax
from jax.experimental import pallas as pl
from jax.experimental.pallas import tpu as pltpu
from jax.sharding import PartitionSpec as P

CHUNK = 256
TILE = 512
GATHERED = 6
F32, BF16 = jnp.float32, jnp.bfloat16


def dot(a, b, contract):
    return lax.dot_general(a, b, (contract, ((), ())), preferred_element_type=F32)


def scale_of(wide):
    return lax.rsqrt(jnp.mean(wide * wide, -1, keepdims=True) + 1e-6)


def forward_kernel(x_ref, wg_ref, wu_ref, wd_ref, h_ref, hid):
    wide = x_ref[...].astype(F32)
    a = (wide * scale_of(wide)).astype(BF16)
    for at in range(0, hid.shape[1], CHUNK):
        gate = dot(a, wg_ref[0, :, at : at + CHUNK], ((1,), (0,)))
        up = dot(a, wu_ref[0, :, at : at + CHUNK], ((1,), (0,)))
        hid[:, at : at + CHUNK] = (gate * (0.5 * jnp.tanh(0.5 * gate) + 0.5) * up).astype(BF16)
    out = dot(hid[...], wd_ref[0], ((1,), (0,))).astype(BF16)
    h_ref[...] = (wide + out.astype(F32)).astype(BF16)


def forward(number, x, wg, wu, wd):
    tokens, d = x.shape
    whole = lambda w: pl.BlockSpec((1, *w.shape[1:]), lambda i: (number, 0, 0))
    rows = pl.BlockSpec((min(TILE, tokens), d), lambda i: (i, 0))
    return pl.pallas_call(
        forward_kernel,
        grid=(tokens // min(TILE, tokens),),
        in_specs=[rows, whole(wg), whole(wu), whole(wd)],
        out_specs=rows,
        out_shape=jax.ShapeDtypeStruct(x.shape, BF16),
        scratch_shapes=[pltpu.VMEM((min(TILE, tokens), wg.shape[2]), BF16)],
        compiler_params=pltpu.CompilerParams(dimension_semantics=("arbitrary",), vmem_limit_bytes=48 * 2**20),
        name="forward",
    )(x, wg, wu, wd)


def train_kernel(
    n, layers, per_layer, gathered, comm,
    x_hbm, h_hbm, dy_hbm, wg_hbm, wu_hbm, wd_hbm,
    sum_hbm, low_hbm, high_hbm, norm_hbm,
    h, dy, a, a_t, da, wgu, wd, hid, dgu, g,
    recv_p, recv_1, recv_2, wide_sum, send_1, send_2, red, squares, all_squares,
    load_sem, w_sem, send_sem, recv_sem, keep_sem, norm_send, norm_recv,
):
    tokens, d = h.shape
    tile = min(TILE, tokens)
    tiles = tokens // tile
    chunks = layers * per_layer
    lows = low_hbm.shape[0]
    me = lax.axis_index("dp")
    chip, core = me // 2, me % 2
    chips = n // 2
    right = lax.rem(chip + 1, chips) * 2 + core
    left = lax.rem(chip + chips - 1, chips) * 2 + core
    partner = chip * 2 + 1 - core
    half = g.shape[1] // 2
    shard = half // chips
    part = shard // 2
    mine = pl.multiple_of(core * half, 16)
    theirs = pl.multiple_of((1 - core) * half, 16)

    def at_shard(q):
        return pl.multiple_of(lax.rem(chip + q, chips) * shard, 16)

    def remote(src, dst, c, k, to):
        return pltpu.make_async_remote_copy(
            src_ref=src, dst_ref=dst, send_sem=send_sem.at[c, k], recv_sem=recv_sem.at[c, k],
            device_id={"dp": to}, device_id_type=pl.DeviceIdType.MESH,
        )

    def load_weights(it, slot):
        layer, j = layers - 1 - it // per_layer, lax.rem(it, per_layer)
        columns = pl.ds(pl.multiple_of(j * CHUNK, CHUNK), CHUNK)
        return (
            pltpu.make_async_copy(wg_hbm.at[layer, :, columns], wgu.at[slot, :, pl.ds(0, CHUNK)], w_sem.at[slot, 0]),
            pltpu.make_async_copy(wu_hbm.at[layer, :, columns], wgu.at[slot, :, pl.ds(CHUNK, CHUNK)], w_sem.at[slot, 1]),
            pltpu.make_async_copy(wd_hbm.at[layer, columns, :], wd.at[slot], w_sem.at[slot, 2]),
        )

    def pair(c, slot):
        return remote(g.at[slot, pl.ds(theirs, half)], recv_p.at[c], c, 0, partner)

    def first(c, slot, k):
        return remote(send_1.at[slot, k], recv_1.at[c, k], c, 1 + k, (right, left)[k])

    def second(c, slot, k):
        return remote(send_2.at[slot, k], recv_2.at[c, k], c, 3 + k, (right, left)[k])

    def spread(c, slot, k):
        rows = pl.ds(mine + at_shard(0), shard)
        return remote(red.at[slot], sum_hbm.at[c, rows], c, 5 + k, (right, left)[k])

    def keep(c, slot, which):
        to = (sum_hbm.at[c, pl.ds(mine + at_shard(0), shard)], low_hbm.at[c - gathered], high_hbm.at[c - gathered - lows])[which]
        return pltpu.make_async_copy(red.at[slot], to, keep_sem.at[c])

    def forward_on(c, k):
        rows = pl.ds(mine + at_shard((chips - 1, 1)[k]) + k * part, part)
        return remote(sum_hbm.at[c, rows], sum_hbm.at[c, rows], c, 7 + k, (right, left)[k])

    def pair_back(c):
        rows = pl.ds(mine, half)
        return remote(sum_hbm.at[c, rows], sum_hbm.at[c, rows], c, 9, partner)

    others = [lax.rem(me + k, n) for k in range(1, n)]
    if comm:
        barrier = pltpu.get_barrier_semaphore()
        for other in others:
            pl.semaphore_signal(barrier, inc=1, device_id={"dp": other}, device_id_type=pl.DeviceIdType.MESH)

    loads = [pltpu.make_async_copy(src, dst, load_sem.at[i]) for i, (src, dst) in enumerate([(h_hbm, h), (dy_hbm, dy)])]
    for load in loads:
        load.start()
    for load in load_weights(0, 0):
        load.start()
    squares[...] = jnp.zeros_like(squares)
    if comm:
        pl.semaphore_wait(barrier, n - 1)
    loads[0].wait()

    def prepare():
        def body(t, _):
            rows = pl.ds(pl.multiple_of(t * tile, tile), tile)
            wide = h[rows, :].astype(F32)
            normed = (wide * scale_of(wide)).astype(BF16)
            a[rows, :] = normed
            a_t[:, rows] = normed.T
            return 0

        lax.fori_loop(0, tiles, body, 0)

    prepare()
    da[...] = jnp.zeros_like(da)
    loads[1].wait()

    def next_layer():
        def body(t, _):
            rows = pl.ds(pl.multiple_of(t * tile, tile), tile)
            wide, by_a = h[rows, :].astype(F32), da[rows, :].astype(BF16).astype(F32)
            scale = scale_of(wide)
            inner = jnp.sum(by_a * wide, -1, keepdims=True)
            by_h = (by_a * scale - wide * (scale * scale * scale * inner * (1.0 / d))).astype(BF16)
            dy[rows, :] = (dy[rows, :].astype(F32) + by_h.astype(F32)).astype(BF16)
            return 0

        lax.fori_loop(0, tiles, body, 0)
        load = pltpu.make_async_copy(x_hbm, h, load_sem.at[0])
        load.start()
        load.wait()
        prepare()

    def compute_hidden(it):
        slot = lax.rem(it, 2)
        for load in load_weights(it, slot):
            load.wait()

        @pl.when(it + 1 < chunks)
        def _():
            for load in load_weights(it + 1, 1 - slot):
                load.start()

        def products(t):
            rows = slice(t * tile, (t + 1) * tile)
            return dot(a[rows, :], wgu[slot], ((1,), (0,))), dot(dy[rows, :], wd[slot], ((1,), (1,)))

        ready = products(0)
        for t in range(tiles):
            (both, by_hid), rows = ready, slice(t * tile, (t + 1) * tile)
            if t + 1 < tiles:
                ready = products(t + 1)
            by_hid = by_hid.astype(BF16).astype(F32)
            gate, up = both[:, :CHUNK], both[:, CHUNK:]
            sig = 0.5 * jnp.tanh(0.5 * gate) + 0.5
            act = gate * sig
            hid[rows, :] = (act * up).astype(BF16)
            dgu[rows, :CHUNK] = (by_hid * up * (sig + act * (1.0 - sig))).astype(BF16)
            dgu[rows, CHUNK:] = (by_hid * act).astype(BF16)

        @pl.when(it < (layers - 1) * per_layer)
        def _():
            def body(t, _):
                rows = pl.ds(pl.multiple_of(t * tile, tile), tile)
                da[rows, :] += dot(dgu[rows, :], wgu[slot], ((1,), (1,)))
                return 0

            lax.fori_loop(0, tiles, body, 0)

    def compute_weights(it):
        slot = lax.rem(it, 2)
        by_wd = dot(hid[...], dy[...], ((0,), (0,))).astype(BF16)
        for k in range(d // CHUNK):
            g[slot, 2 * d + k * CHUNK : 2 * d + (k + 1) * CHUNK, :] = by_wd[:, k * CHUNK : (k + 1) * CHUNK]
        by_wgu = dot(a_t[...], dgu[...], ((1,), (0,))).astype(BF16)
        g[slot, :d, :] = by_wgu[:, :CHUNK]
        g[slot, d : 2 * d, :] = by_wgu[:, CHUNK:]

    def among(c, first_chunk, end, act):
        pl.when((c >= first_chunk) & (c < end))(lambda: act(c, lax.rem(c, 2)))

    def summed(c, slot):
        pair(c, slot).wait()
        wide_sum[lax.rem(c, 3)] = g[slot, pl.ds(mine, half), :].astype(F32) + recv_p[c].astype(F32)
        for k in range(2):
            send_1[slot, k] = wide_sum[lax.rem(c, 3), pl.ds(at_shard(2) + k * part, part), :].astype(BF16)
            first(c, slot, k).start()

    def passed_on(c, slot):
        for k in range(2):
            first(c, slot, k).wait()
        for k, q in enumerate((1, chips - 1)):
            rows = wide_sum[lax.rem(c, 3), pl.ds(at_shard(q), shard), :]
            extra = recv_1[c, k].astype(F32)
            send_2[slot, k, k * part : (k + 1) * part] = (rows[k * part : (k + 1) * part] + extra).astype(BF16)
            send_2[slot, k, (1 - k) * part : (2 - k) * part] = rows[(1 - k) * part : (2 - k) * part].astype(BF16)
            second(c, slot, k).start()

    def finished(c, slot):
        for k in range(2):
            second(c, slot, k).wait()
        total = wide_sum[lax.rem(c, 3), pl.ds(at_shard(0), shard), :]
        total = (total + recv_2[c, 0].astype(F32) + recv_2[c, 1].astype(F32)).astype(BF16)
        red[slot] = total

        @pl.when(c < gathered)
        def _():
            spread(c, slot, 0).start()
            spread(c, slot, 1).start()

        kept(c, lambda which: keep(c, slot, which).start())
        total = total.astype(F32)
        squares[...] += jnp.sum((total * total).reshape(shard // 8, 8, CHUNK), 0)

    def kept(c, act):
        pl.when(c < gathered)(lambda: act(0))
        pl.when((c >= gathered) & (c < gathered + lows))(lambda: act(1))
        pl.when(c >= gathered + lows)(lambda: act(2))

    def spread_on(c, slot):
        kept(c, lambda which: keep(c, slot, which).wait())

        @pl.when(c < gathered)
        def _():
            for k in range(2):
                spread(c, slot, k).wait()
            for k in range(2):
                forward_on(c, k).start()

    def returned(c, slot):
        for k in range(2):
            forward_on(c, k).wait()
        pair_back(c).start()

    def serve_start(it):
        among(it - 3, 0, chunks, passed_on)
        among(it - 6, 0, chunks, spread_on)

    def serve_middle(it):
        among(it - 4, 0, chunks, finished)
        among(it - 1, 0, chunks, summed)
        among(it - 7, 0, gathered, returned)
        among(it - 8, 0, gathered, lambda c, slot: pair_back(c).wait())

    def step(it, _):
        if comm:
            serve_start(it)
        pl.when(it == (layers - 1) * per_layer)(next_layer)
        pl.when(it < chunks)(lambda: compute_hidden(it))
        if comm:
            serve_middle(it)
        pl.when(it < chunks)(lambda: compute_weights(it))
        if comm:
            pl.when(it < chunks)(lambda: pair(it, lax.rem(it, 2)).start())
        return 0

    lax.fori_loop(0, max(chunks + 7, gathered + 9) if comm else chunks, step, 0)

    if comm:
        all_squares[pl.ds(me, 1)] = squares[...][None]
        sends = [
            pltpu.make_async_remote_copy(
                src_ref=squares, dst_ref=all_squares.at[me], send_sem=norm_send.at[k], recv_sem=norm_recv.at[k],
                device_id={"dp": other}, device_id_type=pl.DeviceIdType.MESH,
            )
            for k, other in enumerate(others)
        ]
        for send in sends:
            send.start()
        for send in sends:
            send.wait()
        total = all_squares[0]
        for k in range(1, n):
            total += all_squares[k]
        norm_hbm[...] = total
    else:
        norm_hbm[...] = squares[...]
        pltpu.sync_copy(g.at[0], sum_hbm.at[0])


def train(n, x, h, dy, wg, wu, wd, gathered, comm=True):
    tokens, d = x.shape
    layers, _, ff = wg.shape
    per_layer = ff // CHUNK
    chunks, rows = layers * per_layer, 3 * d
    half = rows // 2
    shard = half // (n // 2)
    part = shard // 2
    lows = (chunks - gathered + 1) // 2
    hbm = pl.BlockSpec(memory_space=pl.ANY)
    vmem = pltpu.VMEM
    dma = pltpu.SemaphoreType.DMA
    return pl.pallas_call(
        functools.partial(train_kernel, n, layers, per_layer, gathered, comm),
        in_specs=[hbm] * 6,
        out_specs=[hbm, hbm, hbm, pl.BlockSpec(memory_space=pltpu.VMEM)],
        out_shape=[jax.ShapeDtypeStruct((k, r, CHUNK), BF16) for k, r in ((gathered, rows), (lows, shard), (chunks - gathered - lows, shard))]
        + [jax.ShapeDtypeStruct((8, CHUNK), F32)],
        scratch_shapes=[
            vmem((tokens, d), BF16), vmem((tokens, d), BF16), vmem((tokens, d), BF16), vmem((d, tokens), BF16), vmem((tokens, d), F32),
            vmem((2, d, 2 * CHUNK), BF16), vmem((2, CHUNK, d), BF16), vmem((tokens, CHUNK), BF16), vmem((tokens, 2 * CHUNK), BF16),
            vmem((2, rows, CHUNK), BF16),
            vmem((chunks, half, CHUNK), BF16), vmem((chunks, 2, part, CHUNK), BF16), vmem((chunks, 2, shard, CHUNK), BF16),
            vmem((3, half, CHUNK), F32), vmem((2, 2, part, CHUNK), BF16), vmem((2, 2, shard, CHUNK), BF16), vmem((2, shard, CHUNK), BF16),
            vmem((8, CHUNK), F32), vmem((n, 8, CHUNK), F32),
            dma((2,)), dma((2, 3)), dma((chunks, 10)), dma((chunks, 10)), dma((chunks,)), dma((n - 1,)), dma((n - 1,)),
        ],
        compiler_params=pltpu.CompilerParams(collective_id=0 if comm else None, has_side_effects=True, vmem_limit_bytes=63 * 2**20),
        cost_estimate=pl.CostEstimate(flops=14 * tokens * d * ff * layers, bytes_accessed=60 * 2**20, transcendentals=0),
        name="train",
    )(x, h, dy, wg, wu, wd)


def adamw_kernel(count, pieces, squares_ref, *refs):
    w, m, v = (refs[pieces + i : pieces + i + 3] for i in (0, 3, 6))
    rest = refs[pieces + 9 :]
    if pieces == 1:
        g, rest = refs[0].at[0], rest[-9:]
    else:
        g, rest = rest[-1], rest[-10:-1]
        me = lax.axis_index("dp")
        chips, shard = pieces // 2, refs[0].shape[1]
        for i in range(pieces):
            core = (me + i // chips) % 2
            at = core * (chips * shard) + lax.rem(me // 2 + (0, chips - 1, 1, 2)[i % chips], chips) * shard
            g[pl.ds(pl.multiple_of(at, 16), shard), :] = refs[i][0]
    new_w, new_m, new_v = rest[:3], rest[3:6], rest[6:]
    total = jnp.sum(squares_ref[...], (0, 1), keepdims=True)
    factor = jnp.minimum(1.0, 0.5 * lax.rsqrt(total / count + 1e-30))
    d = w[0].shape[1]
    for i in range(3):
        if i < 2:
            grad = g[i * d : (i + 1) * d, :]
        else:
            grad = jnp.concatenate([g[2 * d + k : 2 * d + k + CHUNK, :] for k in range(0, d, CHUNK)], 1)
        grad = grad.astype(F32) * factor
        mean = 0.9 * m[i][0] + 0.1 * grad
        square = 0.95 * v[i][0] + 0.05 * grad * grad
        wide = w[i][0].astype(F32)
        new_w[i][0] = (wide - 0.02 * (mean * lax.rsqrt(square + 1e-8) + 0.1 * wide)).astype(BF16)
        new_m[i][0] = mean
        new_v[i][0] = square


def adamw(start, end, squares, gradients, weights, m, v, so_far):
    layers, d, ff = weights[0].shape
    per_layer = ff // CHUNK
    chunks, pieces = end - start, len(gradients)
    skip = start if pieces == 1 else 0
    layer = lambda i: layers - 1 - (start + i) // per_layer
    across = pl.BlockSpec((1, d, CHUNK), lambda i: (layer(i), 0, (start + i) % per_layer))
    down = pl.BlockSpec((1, CHUNK, d), lambda i: (layer(i), (start + i) % per_layer, 0))
    each = [across, across, down] * 3
    count = sum(w.size for w in weights)
    carried = list(so_far or [])
    return pl.pallas_call(
        functools.partial(adamw_kernel, count, pieces),
        grid=(chunks,),
        in_specs=[pl.BlockSpec((8, CHUNK), lambda i: (0, 0))]
        + [pl.BlockSpec((1, *g.shape[1:]), lambda i: (skip + i, 0, 0)) for g in gradients]
        + each
        + [pl.BlockSpec(memory_space=pl.ANY)] * len(carried),
        out_specs=each,
        out_shape=[jax.ShapeDtypeStruct(t.shape, t.dtype) for t in (*weights, *m, *v)],
        scratch_shapes=[] if pieces == 1 else [pltpu.VMEM((3 * d, CHUNK), BF16)],
        input_output_aliases={10 + pieces + i: i for i in range(len(carried))},
        compiler_params=pltpu.CompilerParams(dimension_semantics=("arbitrary",), vmem_limit_bytes=62 * 2**20),
        cost_estimate=pl.CostEstimate(flops=chunks * FLOPS_OF_A_CHUNK, bytes_accessed=chunks * 66 * d * CHUNK, transcendentals=0),
        name=f"adamw_{start}",
    )(squares, *gradients, *weights, *m, *v, *carried)


FLOPS_OF_A_CHUNK = 10**10


def solution(mesh):
    n = mesh.shape["dp"]
    chips = n // 2
    right = [(2 * c + k, (2 * c + 2) % n + k) for c in range(chips) for k in range(2)]
    left = [(to, source) for source, to in right]
    pairs = [(i, i ^ 1) for i in range(n)]

    def go(t, way):
        return lax.ppermute(t, "dp", way)

    def step(x, dy, *arrays):
        weights, m, v = (arrays[i : i + 3] for i in (0, 3, 6))
        h = forward(0, x[0], *weights)
        g, low, high, squares = train(n, x[0], h, dy[0], *weights, GATHERED)
        take = lambda first, end, parts, so_far: adamw(first, end, squares, parts, weights, m, v, so_far)
        lows = [low, go(low, right), go(low, left)]
        highs = [high, go(high, right), go(high, left)]
        low_pairs = [go(low, pairs)]
        high_pairs = [go(high, pairs)]
        new = take(0, GATHERED // 2, [g], None)
        lows, new = lax.optimization_barrier((lows, new))
        lows.append(go(lows[1], right))
        low_pairs += [go(t, pairs) for t in lows[1:3]]
        new = take(GATHERED // 2, GATHERED, [g], new)
        lows, highs, low_pairs, new = lax.optimization_barrier((lows, highs, low_pairs, new))
        highs.append(go(highs[2], left))
        low_pairs.append(go(lows[3], pairs))
        high_pairs += [go(t, pairs) for t in highs[1:3]]
        end = GATHERED + low.shape[0]
        new = take(GATHERED, end, lows + low_pairs, new)
        highs, high_pairs, new = lax.optimization_barrier((highs, high_pairs, new))
        high_pairs.append(go(highs[3], pairs))
        return tuple(take(end, end + high.shape[0], highs + high_pairs, new))

    return jax.shard_map(
        step,
        mesh=mesh,
        in_specs=(P(("rep", "dp"), None, None),) * 2 + (P(None, None, None),) * 9,
        out_specs=(P("rep", None, None),) * 9,
        check_vma=False,
    )
```

```python
import functools

import jax
import jax.numpy as jnp
from jax import lax
from jax.experimental import pallas as pl
from jax.experimental.pallas import tpu as pltpu
from jax.sharding import PartitionSpec as P

CHUNK = 256
TILE = 512
GATHERED = 6
F32, BF16 = jnp.float32, jnp.bfloat16


def dot(a, b, contract):
    return lax.dot_general(a, b, (contract, ((), ())), preferred_element_type=F32)


def scale_of(wide):
    return lax.rsqrt(jnp.mean(wide * wide, -1, keepdims=True) + 1e-6)


def forward_kernel(x_ref, wg_ref, wu_ref, wd_ref, h_ref, hid):
    wide = x_ref[...].astype(F32)
    a = (wide * scale_of(wide)).astype(BF16)
    for at in range(0, hid.shape[1], CHUNK):
        gate = dot(a, wg_ref[0, :, at : at + CHUNK], ((1,), (0,)))
        up = dot(a, wu_ref[0, :, at : at + CHUNK], ((1,), (0,)))
        hid[:, at : at + CHUNK] = (gate * (0.5 * jnp.tanh(0.5 * gate) + 0.5) * up).astype(BF16)
    out = dot(hid[...], wd_ref[0], ((1,), (0,))).astype(BF16)
    h_ref[...] = (wide + out.astype(F32)).astype(BF16)


def forward(number, x, wg, wu, wd):
    tokens, d = x.shape
    whole = lambda w: pl.BlockSpec((1, *w.shape[1:]), lambda i: (number, 0, 0))
    rows = pl.BlockSpec((min(TILE, tokens), d), lambda i: (i, 0))
    return pl.pallas_call(
        forward_kernel,
        grid=(tokens // min(TILE, tokens),),
        in_specs=[rows, whole(wg), whole(wu), whole(wd)],
        out_specs=rows,
        out_shape=jax.ShapeDtypeStruct(x.shape, BF16),
        scratch_shapes=[pltpu.VMEM((min(TILE, tokens), wg.shape[2]), BF16)],
        compiler_params=pltpu.CompilerParams(dimension_semantics=("arbitrary",), vmem_limit_bytes=48 * 2**20),
        name="forward",
    )(x, wg, wu, wd)


def train_kernel(
    n, layers, per_layer, gathered, comm,
    x_hbm, h_hbm, dy_hbm, wg_hbm, wu_hbm, wd_hbm,
    sum_hbm, low_hbm, high_hbm, norm_hbm,
    x, h, dy, a, a_t, da, wgu, wd, hid, dgu, g,
    recv_p, recv_1, recv_2, send_1, send_2, red, squares, all_squares,
    load_sem, w_sem, send_sem, recv_sem, keep_sem, norm_send, norm_recv,
):
    tokens, d = h.shape
    tile = min(TILE, tokens)
    tiles = tokens // tile
    chunks = layers * per_layer
    lows = low_hbm.shape[0]
    me = lax.axis_index("dp")
    chip, core = me // 2, me % 2
    chips = n // 2
    right = lax.rem(chip + 1, chips) * 2 + core
    left = lax.rem(chip + chips - 1, chips) * 2 + core
    partner = chip * 2 + 1 - core
    half = g.shape[1] // 2
    shard = half // chips
    part = shard // 2
    mine = pl.multiple_of(core * half, 16)
    theirs = pl.multiple_of((1 - core) * half, 16)

    def at_shard(q):
        return pl.multiple_of(lax.rem(chip + q, chips) * shard, 16)

    def remote(src, dst, c, k, to):
        return pltpu.make_async_remote_copy(
            src_ref=src, dst_ref=dst, send_sem=send_sem.at[c, k], recv_sem=recv_sem.at[c, k],
            device_id={"dp": to}, device_id_type=pl.DeviceIdType.MESH,
        )

    def load_weights(it, slot):
        layer, j = layers - 1 - it // per_layer, lax.rem(it, per_layer)
        columns = pl.ds(pl.multiple_of(j * CHUNK, CHUNK), CHUNK)
        return (
            pltpu.make_async_copy(wg_hbm.at[layer, :, columns], wgu.at[slot, :, pl.ds(0, CHUNK)], w_sem.at[slot, 0]),
            pltpu.make_async_copy(wu_hbm.at[layer, :, columns], wgu.at[slot, :, pl.ds(CHUNK, CHUNK)], w_sem.at[slot, 1]),
            pltpu.make_async_copy(wd_hbm.at[layer, columns, :], wd.at[slot], w_sem.at[slot, 2]),
        )

    def pair(c, slot):
        return remote(g.at[lax.rem(c, 4), pl.ds(theirs, half)], recv_p.at[c], c, 0, partner)

    def first(c, slot, k):
        return remote(send_1.at[slot, k], recv_1.at[c, k], c, 1 + k, (right, left)[k])

    def second(c, slot, k):
        return remote(send_2.at[slot, k], recv_2.at[c, k], c, 3 + k, (right, left)[k])

    def spread(c, slot, k):
        rows = pl.ds(mine + at_shard(0), shard)
        return remote(red.at[slot], sum_hbm.at[c, rows], c, 5 + k, (right, left)[k])

    def keep(c, slot, which):
        to = (sum_hbm.at[c, pl.ds(mine + at_shard(0), shard)], low_hbm.at[c - gathered], high_hbm.at[c - gathered - lows])[which]
        return pltpu.make_async_copy(red.at[slot], to, keep_sem.at[c])

    def forward_on(c, k):
        rows = pl.ds(mine + at_shard((chips - 1, 1)[k]) + k * part, part)
        return remote(sum_hbm.at[c, rows], sum_hbm.at[c, rows], c, 7 + k, (right, left)[k])

    def pair_back(c):
        rows = pl.ds(mine, half)
        return remote(sum_hbm.at[c, rows], sum_hbm.at[c, rows], c, 9, partner)

    others = [lax.rem(me + k, n) for k in range(1, n)]
    if comm:
        barrier = pltpu.get_barrier_semaphore()
        for other in others:
            pl.semaphore_signal(barrier, inc=1, device_id={"dp": other}, device_id_type=pl.DeviceIdType.MESH)

    loads = [pltpu.make_async_copy(src, dst, load_sem.at[i]) for i, (src, dst) in enumerate([(h_hbm, h), (dy_hbm, dy), (x_hbm, x)])]
    loads[0].start()
    for load in load_weights(0, 0):
        load.start()
    loads[1].start()
    loads[2].start()
    squares[...] = jnp.zeros_like(squares)
    if comm:
        pl.semaphore_wait(barrier, n - 1)
    loads[0].wait()

    def prepare(h):
        def body(t, _):
            rows = pl.ds(pl.multiple_of(t * tile, tile), tile)
            wide = h[rows, :].astype(F32)
            normed = (wide * scale_of(wide)).astype(BF16)
            a[rows, :] = normed
            a_t[:, rows] = normed.T
            return 0

        lax.fori_loop(0, tiles, body, 0)

    prepare(h)
    da[...] = jnp.zeros_like(da)
    loads[1].wait()

    def next_layer():
        def body(t, _):
            rows = pl.ds(pl.multiple_of(t * tile, tile), tile)
            wide, by_a = h[rows, :].astype(F32), da[rows, :].astype(BF16).astype(F32)
            scale = scale_of(wide)
            inner = jnp.sum(by_a * wide, -1, keepdims=True)
            by_h = (by_a * scale - wide * (scale * scale * scale * inner * (1.0 / d))).astype(BF16)
            dy[rows, :] = (dy[rows, :].astype(F32) + by_h.astype(F32)).astype(BF16)
            return 0

        lax.fori_loop(0, tiles, body, 0)
        loads[2].wait()
        prepare(x)

    def compute_hidden(it):
        slot = lax.rem(it, 2)
        for load in load_weights(it, slot):
            load.wait()

        @pl.when(it + 1 < chunks)
        def _():
            for load in load_weights(it + 1, 1 - slot):
                load.start()

        def products(t):
            rows = slice(t * tile, (t + 1) * tile)
            return dot(a[rows, :], wgu[slot], ((1,), (0,))), dot(dy[rows, :], wd[slot], ((1,), (1,)))

        ready = products(0)
        for t in range(tiles):
            (both, by_hid), rows = ready, slice(t * tile, (t + 1) * tile)
            if t + 1 < tiles:
                ready = products(t + 1)
            by_hid = by_hid.astype(BF16).astype(F32)
            gate, up = both[:, :CHUNK], both[:, CHUNK:]
            sig = 0.5 * jnp.tanh(0.5 * gate) + 0.5
            act = gate * sig
            hid[rows, :] = (act * up).astype(BF16)
            dgu[rows, :CHUNK] = (by_hid * up * (sig + act * (1.0 - sig))).astype(BF16)
            dgu[rows, CHUNK:] = (by_hid * act).astype(BF16)

        @pl.when(it < (layers - 1) * per_layer)
        def _():
            for rows in (slice(0, tokens // 2), slice(tokens // 2, tokens)):
                da[rows, :] += dot(dgu[rows, :], wgu[slot], ((1,), (1,)))

    def compute_weights(it):
        slot = lax.rem(it, 4)
        by_wd = dot(hid[...], dy[...], ((0,), (0,))).astype(BF16)
        for k in range(d // CHUNK):
            g[slot, 2 * d + k * CHUNK : 2 * d + (k + 1) * CHUNK, :] = by_wd[:, k * CHUNK : (k + 1) * CHUNK]
        by_wgu = dot(a_t[...], dgu[...], ((1,), (0,))).astype(BF16)
        g[slot, :d, :] = by_wgu[:, :CHUNK]
        g[slot, d : 2 * d, :] = by_wgu[:, CHUNK:]

    def among(c, first_chunk, end, act):
        pl.when((c >= first_chunk) & (c < end))(lambda: act(c, lax.rem(c, 2)))

    def of_pair(c, at, rows):
        at = pl.multiple_of(at, 16)
        return g[lax.rem(c, 4), pl.ds(mine + at, rows), :].astype(F32) + recv_p[c, pl.ds(at, rows), :].astype(F32)

    def summed(c, slot):
        pair(c, slot).wait()
        for k in range(2):
            send_1[slot, k] = of_pair(c, at_shard(2) + k * part, part).astype(BF16)
            first(c, slot, k).start()

    def passed_on(c, slot):
        for k in range(2):
            first(c, slot, k).wait()
        for k, q in enumerate((1, chips - 1)):
            rows = of_pair(c, at_shard(q), shard)
            extra = recv_1[c, k].astype(F32)
            send_2[slot, k, k * part : (k + 1) * part] = (rows[k * part : (k + 1) * part] + extra).astype(BF16)
            send_2[slot, k, (1 - k) * part : (2 - k) * part] = rows[(1 - k) * part : (2 - k) * part].astype(BF16)
            second(c, slot, k).start()

    def finished(c, slot):
        for k in range(2):
            second(c, slot, k).wait()
        total = of_pair(c, at_shard(0), shard)
        total = (total + recv_2[c, 0].astype(F32) + recv_2[c, 1].astype(F32)).astype(BF16)
        red[slot] = total

        @pl.when(c < gathered)
        def _():
            spread(c, slot, 0).start()
            spread(c, slot, 1).start()

        kept(c, lambda which: keep(c, slot, which).start())
        total = total.astype(F32)
        squares[...] += jnp.sum((total * total).reshape(shard // 8, 8, CHUNK), 0)

    def kept(c, act):
        pl.when(c < gathered)(lambda: act(0))
        pl.when((c >= gathered) & (c < gathered + lows))(lambda: act(1))
        pl.when(c >= gathered + lows)(lambda: act(2))

    def spread_on(c, slot):
        kept(c, lambda which: keep(c, slot, which).wait())

        @pl.when(c < gathered)
        def _():
            for k in range(2):
                spread(c, slot, k).wait()
            for k in range(2):
                forward_on(c, k).start()

    def returned(c, slot):
        for k in range(2):
            forward_on(c, k).wait()
        pair_back(c).start()

    def serve_start(it):
        among(it - 3, 0, chunks, passed_on)
        among(it - 6, 0, chunks, spread_on)

    def serve_middle(it):
        among(it - 4, 0, chunks, finished)
        among(it - 1, 0, chunks, summed)
        among(it - 7, 0, gathered, returned)
        among(it - 8, 0, gathered, lambda c, slot: pair_back(c).wait())

    def step(it, _):
        if comm:
            serve_start(it)
        pl.when(it == (layers - 1) * per_layer)(next_layer)
        pl.when(it < chunks)(lambda: compute_hidden(it))
        if comm:
            serve_middle(it)
        pl.when(it < chunks)(lambda: compute_weights(it))
        if comm:
            pl.when(it < chunks)(lambda: pair(it, lax.rem(it, 2)).start())
        return 0

    lax.fori_loop(0, max(chunks + 7, gathered + 9) if comm else chunks, step, 0)

    if comm:
        all_squares[pl.ds(me, 1)] = squares[...][None]
        sends = [
            pltpu.make_async_remote_copy(
                src_ref=squares, dst_ref=all_squares.at[me], send_sem=norm_send.at[k], recv_sem=norm_recv.at[k],
                device_id={"dp": other}, device_id_type=pl.DeviceIdType.MESH,
            )
            for k, other in enumerate(others)
        ]
        for send in sends:
            send.start()
        for send in sends:
            send.wait()
        total = all_squares[0]
        for k in range(1, n):
            total += all_squares[k]
        norm_hbm[...] = total
    else:
        norm_hbm[...] = squares[...]
        pltpu.sync_copy(g.at[0], sum_hbm.at[0])


def train(n, x, h, dy, wg, wu, wd, gathered, comm=True):
    tokens, d = x.shape
    layers, _, ff = wg.shape
    per_layer = ff // CHUNK
    chunks, rows = layers * per_layer, 3 * d
    half = rows // 2
    shard = half // (n // 2)
    part = shard // 2
    lows = (chunks - gathered + 1) // 2
    hbm = pl.BlockSpec(memory_space=pl.ANY)
    vmem = pltpu.VMEM
    dma = pltpu.SemaphoreType.DMA
    return pl.pallas_call(
        functools.partial(train_kernel, n, layers, per_layer, gathered, comm),
        in_specs=[hbm] * 6,
        out_specs=[hbm, hbm, hbm, pl.BlockSpec(memory_space=pltpu.VMEM)],
        out_shape=[jax.ShapeDtypeStruct((k, r, CHUNK), BF16) for k, r in ((gathered, rows), (lows, shard), (chunks - gathered - lows, shard))]
        + [jax.ShapeDtypeStruct((8, CHUNK), F32)],
        scratch_shapes=[
            vmem((tokens, d), BF16), vmem((tokens, d), BF16), vmem((tokens, d), BF16), vmem((tokens, d), BF16), vmem((d, tokens), BF16), vmem((tokens, d), F32),
            vmem((2, d, 2 * CHUNK), BF16), vmem((2, CHUNK, d), BF16), vmem((tokens, CHUNK), BF16), vmem((tokens, 2 * CHUNK), BF16),
            vmem((4, rows, CHUNK), BF16),
            vmem((chunks, half, CHUNK), BF16), vmem((chunks, 2, part, CHUNK), BF16), vmem((chunks, 2, shard, CHUNK), BF16),
            vmem((2, 2, part, CHUNK), BF16), vmem((2, 2, shard, CHUNK), BF16), vmem((2, shard, CHUNK), BF16),
            vmem((8, CHUNK), F32), vmem((n, 8, CHUNK), F32),
            dma((3,)), dma((2, 3)), dma((chunks, 10)), dma((chunks, 10)), dma((chunks,)), dma((n - 1,)), dma((n - 1,)),
        ],
        compiler_params=pltpu.CompilerParams(collective_id=0 if comm else None, has_side_effects=True, vmem_limit_bytes=63 * 2**20),
        cost_estimate=pl.CostEstimate(flops=14 * tokens * d * ff * layers, bytes_accessed=60 * 2**20, transcendentals=0),
        name="train",
    )(x, h, dy, wg, wu, wd)


def adamw_kernel(count, pieces, squares_ref, *refs):
    w, m, v = (refs[pieces + i : pieces + i + 3] for i in (0, 3, 6))
    rest = refs[pieces + 9 :]
    if pieces == 1:
        g, rest = refs[0].at[0], rest[-9:]
    else:
        g, rest = rest[-1], rest[-10:-1]
        me = lax.axis_index("dp")
        chips, shard = pieces // 2, refs[0].shape[1]
        for i in range(pieces):
            core = (me + i // chips) % 2
            at = core * (chips * shard) + lax.rem(me // 2 + (0, chips - 1, 1, 2)[i % chips], chips) * shard
            g[pl.ds(pl.multiple_of(at, 16), shard), :] = refs[i][0]
    new_w, new_m, new_v = rest[:3], rest[3:6], rest[6:]
    total = jnp.sum(squares_ref[...], (0, 1), keepdims=True)
    factor = jnp.minimum(1.0, 0.5 * lax.rsqrt(total / count + 1e-30))
    d = w[0].shape[1]
    for i in range(3):
        if i < 2:
            grad = g[i * d : (i + 1) * d, :]
        else:
            grad = jnp.concatenate([g[2 * d + k : 2 * d + k + CHUNK, :] for k in range(0, d, CHUNK)], 1)
        grad = grad.astype(F32) * factor
        mean = 0.9 * m[i][0] + 0.1 * grad
        square = 0.95 * v[i][0] + 0.05 * grad * grad
        wide = w[i][0].astype(F32)
        new_w[i][0] = (wide - 0.02 * (mean * lax.rsqrt(square + 1e-8) + 0.1 * wide)).astype(BF16)
        new_m[i][0] = mean
        new_v[i][0] = square


def adamw(start, end, squares, gradients, weights, m, v, so_far):
    layers, d, ff = weights[0].shape
    per_layer = ff // CHUNK
    chunks, pieces = end - start, len(gradients)
    skip = start if pieces == 1 else 0
    layer = lambda i: layers - 1 - (start + i) // per_layer
    across = pl.BlockSpec((1, d, CHUNK), lambda i: (layer(i), 0, (start + i) % per_layer))
    down = pl.BlockSpec((1, CHUNK, d), lambda i: (layer(i), (start + i) % per_layer, 0))
    each = [across, across, down] * 3
    count = sum(w.size for w in weights)
    carried = list(so_far or [])
    return pl.pallas_call(
        functools.partial(adamw_kernel, count, pieces),
        grid=(chunks,),
        in_specs=[pl.BlockSpec((8, CHUNK), lambda i: (0, 0))]
        + [pl.BlockSpec((1, *g.shape[1:]), lambda i: (skip + i, 0, 0)) for g in gradients]
        + each
        + [pl.BlockSpec(memory_space=pl.ANY)] * len(carried),
        out_specs=each,
        out_shape=[jax.ShapeDtypeStruct(t.shape, t.dtype) for t in (*weights, *m, *v)],
        scratch_shapes=[] if pieces == 1 else [pltpu.VMEM((3 * d, CHUNK), BF16)],
        input_output_aliases={10 + pieces + i: i for i in range(len(carried))},
        compiler_params=pltpu.CompilerParams(dimension_semantics=("arbitrary",), vmem_limit_bytes=62 * 2**20),
        cost_estimate=pl.CostEstimate(flops=chunks * FLOPS_OF_A_CHUNK, bytes_accessed=chunks * 66 * d * CHUNK, transcendentals=0),
        name=f"adamw_{start}",
    )(squares, *gradients, *weights, *m, *v, *carried)


FLOPS_OF_A_CHUNK = 10**10


def solution(mesh):
    n = mesh.shape["dp"]
    chips = n // 2
    right = [(2 * c + k, (2 * c + 2) % n + k) for c in range(chips) for k in range(2)]
    left = [(to, source) for source, to in right]
    pairs = [(i, i ^ 1) for i in range(n)]

    def go(t, way):
        return lax.ppermute(t, "dp", way)

    def step(x, dy, *arrays):
        weights, m, v = (arrays[i : i + 3] for i in (0, 3, 6))
        h = forward(0, x[0], *weights)
        g, low, high, squares = train(n, x[0], h, dy[0], *weights, GATHERED)
        take = lambda first, end, parts, so_far: adamw(first, end, squares, parts, weights, m, v, so_far)
        lows = [low, go(low, right), go(low, left)]
        highs = [high, go(high, right), go(high, left)]
        low_pairs = [go(low, pairs)]
        high_pairs = [go(high, pairs)]
        new = take(0, GATHERED // 2, [g], None)
        lows, new = lax.optimization_barrier((lows, new))
        lows.append(go(lows[1], right))
        low_pairs += [go(t, pairs) for t in lows[1:3]]
        new = take(GATHERED // 2, GATHERED, [g], new)
        lows, highs, low_pairs, new = lax.optimization_barrier((lows, highs, low_pairs, new))
        highs.append(go(highs[2], left))
        low_pairs.append(go(lows[3], pairs))
        high_pairs += [go(t, pairs) for t in highs[1:3]]
        end = GATHERED + low.shape[0]
        new = take(GATHERED, end, lows + low_pairs, new)
        highs, high_pairs, new = lax.optimization_barrier((highs, high_pairs, new))
        high_pairs.append(go(highs[3], pairs))
        return tuple(take(end, end + high.shape[0], highs + high_pairs, new))

    return jax.shard_map(
        step,
        mesh=mesh,
        in_specs=(P(("rep", "dp"), None, None),) * 2 + (P(None, None, None),) * 9,
        out_specs=(P("rep", None, None),) * 9,
        check_vma=False,
    )
```

```python
import functools

import jax
import jax.numpy as jnp
from jax import lax
from jax.experimental import pallas as pl
from jax.experimental.pallas import tpu as pltpu
from jax.sharding import PartitionSpec as P

CHUNK = 256
TILE = 512
GATHERED = 6
F32, BF16 = jnp.float32, jnp.bfloat16


def dot(a, b, contract):
    return lax.dot_general(a, b, (contract, ((), ())), preferred_element_type=F32)


def scale_of(wide):
    return lax.rsqrt(jnp.mean(wide * wide, -1, keepdims=True) + 1e-6)


def forward_kernel(x_ref, wg_ref, wu_ref, wd_ref, h_ref, hid):
    wide = x_ref[...].astype(F32)
    a = (wide * scale_of(wide)).astype(BF16)
    for at in range(0, hid.shape[1], CHUNK):
        gate = dot(a, wg_ref[0, :, at : at + CHUNK], ((1,), (0,)))
        up = dot(a, wu_ref[0, :, at : at + CHUNK], ((1,), (0,)))
        hid[:, at : at + CHUNK] = (gate * (0.5 * jnp.tanh(0.5 * gate) + 0.5) * up).astype(BF16)
    out = dot(hid[...], wd_ref[0], ((1,), (0,))).astype(BF16)
    h_ref[...] = (wide + out.astype(F32)).astype(BF16)


def forward(number, x, wg, wu, wd):
    tokens, d = x.shape
    whole = lambda w: pl.BlockSpec((1, *w.shape[1:]), lambda i: (number, 0, 0))
    rows = pl.BlockSpec((min(1024, tokens), d), lambda i: (i, 0))
    return pl.pallas_call(
        forward_kernel,
        grid=(tokens // min(1024, tokens),),
        in_specs=[rows, whole(wg), whole(wu), whole(wd)],
        out_specs=rows,
        out_shape=jax.ShapeDtypeStruct(x.shape, BF16),
        scratch_shapes=[pltpu.VMEM((min(1024, tokens), wg.shape[2]), BF16)],
        compiler_params=pltpu.CompilerParams(dimension_semantics=("arbitrary",), vmem_limit_bytes=48 * 2**20),
        name="forward",
    )(x, wg, wu, wd)


def train_kernel(
    n, layers, per_layer, gathered, comm,
    x_hbm, h_hbm, dy_hbm, wg_hbm, wu_hbm, wd_hbm,
    sum_hbm, low_hbm, high_hbm, norm_hbm,
    x, h, dy, a, a_t, da, wgu, wd, hid, dgu, g,
    recv_p, recv_1, recv_2, send_1, send_2, red, squares, all_squares,
    load_sem, w_sem, send_sem, recv_sem, keep_sem, norm_send, norm_recv,
):
    tokens, d = h.shape
    tile = min(TILE, tokens)
    tiles = tokens // tile
    chunks = layers * per_layer
    lows = low_hbm.shape[0]
    me = lax.axis_index("dp")
    chip, core = me // 2, me % 2
    chips = n // 2
    right = lax.rem(chip + 1, chips) * 2 + core
    left = lax.rem(chip + chips - 1, chips) * 2 + core
    partner = chip * 2 + 1 - core
    half = g.shape[1] // 2
    shard = half // chips
    part = shard // 2
    mine = pl.multiple_of(core * half, 16)
    theirs = pl.multiple_of((1 - core) * half, 16)

    def at_shard(q):
        return pl.multiple_of(lax.rem(chip + q, chips) * shard, 16)

    def remote(src, dst, c, k, to):
        return pltpu.make_async_remote_copy(
            src_ref=src, dst_ref=dst, send_sem=send_sem.at[c, k], recv_sem=recv_sem.at[c, k],
            device_id={"dp": to}, device_id_type=pl.DeviceIdType.MESH,
        )

    def load_weights(it, slot):
        layer, j = layers - 1 - it // per_layer, lax.rem(it, per_layer)
        columns = pl.ds(pl.multiple_of(j * CHUNK, CHUNK), CHUNK)
        return (
            pltpu.make_async_copy(wg_hbm.at[layer, :, columns], wgu.at[slot, :, pl.ds(0, CHUNK)], w_sem.at[slot, 0]),
            pltpu.make_async_copy(wu_hbm.at[layer, :, columns], wgu.at[slot, :, pl.ds(CHUNK, CHUNK)], w_sem.at[slot, 1]),
            pltpu.make_async_copy(wd_hbm.at[layer, columns, :], wd.at[slot], w_sem.at[slot, 2]),
        )

    def pair(c, slot):
        return remote(g.at[lax.rem(c, 4), pl.ds(theirs, half)], recv_p.at[c], c, 0, partner)

    def first(c, slot, k):
        return remote(send_1.at[slot, k], recv_1.at[c, k], c, 1 + k, (right, left)[k])

    def second(c, slot, k):
        return remote(send_2.at[slot, k], recv_2.at[c, k], c, 3 + k, (right, left)[k])

    def spread(c, slot, k):
        rows = pl.ds(mine + at_shard(0), shard)
        return remote(red.at[slot], sum_hbm.at[c, rows], c, 5 + k, (right, left)[k])

    def keep(c, slot, which):
        to = (sum_hbm.at[c, pl.ds(mine + at_shard(0), shard)], low_hbm.at[c - gathered], high_hbm.at[c - gathered - lows])[which]
        return pltpu.make_async_copy(red.at[slot], to, keep_sem.at[c])

    def forward_on(c, k):
        rows = pl.ds(mine + at_shard((chips - 1, 1)[k]) + k * part, part)
        return remote(sum_hbm.at[c, rows], sum_hbm.at[c, rows], c, 7 + k, (right, left)[k])

    def pair_back(c):
        rows = pl.ds(mine, half)
        return remote(sum_hbm.at[c, rows], sum_hbm.at[c, rows], c, 9, partner)

    others = [lax.rem(me + k, n) for k in range(1, n)]
    if comm:
        barrier = pltpu.get_barrier_semaphore()
        for other in others:
            pl.semaphore_signal(barrier, inc=1, device_id={"dp": other}, device_id_type=pl.DeviceIdType.MESH)

    loads = [pltpu.make_async_copy(src, dst, load_sem.at[i]) for i, (src, dst) in enumerate([(h_hbm, h), (dy_hbm, dy), (x_hbm, x)])]
    loads[0].start()
    for load in load_weights(0, 0):
        load.start()
    loads[1].start()
    loads[2].start()
    squares[...] = jnp.zeros_like(squares)
    if comm:
        pl.semaphore_wait(barrier, n - 1)
    loads[0].wait()

    def prepare(h):
        def body(t, _):
            rows = pl.ds(pl.multiple_of(t * tile, tile), tile)
            wide = h[rows, :].astype(F32)
            normed = (wide * scale_of(wide)).astype(BF16)
            a[rows, :] = normed
            a_t[:, rows] = normed.T
            return 0

        lax.fori_loop(0, tiles, body, 0)

    prepare(h)
    da[...] = jnp.zeros_like(da)
    loads[1].wait()

    def next_layer():
        def body(t, _):
            rows = pl.ds(pl.multiple_of(t * tile, tile), tile)
            wide, by_a = h[rows, :].astype(F32), da[rows, :].astype(BF16).astype(F32)
            scale = scale_of(wide)
            inner = jnp.sum(by_a * wide, -1, keepdims=True)
            by_h = (by_a * scale - wide * (scale * scale * scale * inner * (1.0 / d))).astype(BF16)
            dy[rows, :] = (dy[rows, :].astype(F32) + by_h.astype(F32)).astype(BF16)
            return 0

        lax.fori_loop(0, tiles, body, 0)
        loads[2].wait()
        prepare(x)

    def compute_hidden(it):
        slot = lax.rem(it, 2)
        for load in load_weights(it, slot):
            load.wait()

        @pl.when(it + 1 < chunks)
        def _():
            for load in load_weights(it + 1, 1 - slot):
                load.start()

        def products(t):
            rows = slice(t * tile, (t + 1) * tile)
            return dot(a[rows, :], wgu[slot], ((1,), (0,))), dot(dy[rows, :], wd[slot], ((1,), (1,)))

        ready = products(0)
        for t in range(tiles):
            (both, by_hid), rows = ready, slice(t * tile, (t + 1) * tile)
            if t + 1 < tiles:
                ready = products(t + 1)
            by_hid = by_hid.astype(BF16).astype(F32)
            gate, up = both[:, :CHUNK], both[:, CHUNK:]
            sig = 0.5 * jnp.tanh(0.5 * gate) + 0.5
            act = gate * sig
            hid[rows, :] = (act * up).astype(BF16)
            dgu[rows, :CHUNK] = (by_hid * up * (sig + act * (1.0 - sig))).astype(BF16)
            dgu[rows, CHUNK:] = (by_hid * act).astype(BF16)

        @pl.when(it < (layers - 1) * per_layer)
        def _():
            for rows in (slice(0, tokens // 2), slice(tokens // 2, tokens)):
                da[rows, :] += dot(dgu[rows, :], wgu[slot], ((1,), (1,)))

    def compute_weights(it):
        slot = lax.rem(it, 4)
        by_wd = dot(hid[...], dy[...], ((0,), (0,))).astype(BF16)
        for k in range(d // CHUNK):
            g[slot, 2 * d + k * CHUNK : 2 * d + (k + 1) * CHUNK, :] = by_wd[:, k * CHUNK : (k + 1) * CHUNK]
        by_wgu = dot(a_t[...], dgu[...], ((1,), (0,))).astype(BF16)
        g[slot, :d, :] = by_wgu[:, :CHUNK]
        g[slot, d : 2 * d, :] = by_wgu[:, CHUNK:]

    def among(c, first_chunk, end, act):
        pl.when((c >= first_chunk) & (c < end))(lambda: act(c, lax.rem(c, 2)))

    def of_pair(c, at, rows):
        at = pl.multiple_of(at, 16)
        return g[lax.rem(c, 4), pl.ds(mine + at, rows), :].astype(F32) + recv_p[c, pl.ds(at, rows), :].astype(F32)

    def summed(c, slot):
        pair(c, slot).wait()
        for k in range(2):
            send_1[slot, k] = of_pair(c, at_shard(2) + k * part, part).astype(BF16)
            first(c, slot, k).start()

    def passed_on(c, slot):
        for k in range(2):
            first(c, slot, k).wait()
        for k, q in enumerate((1, chips - 1)):
            rows = of_pair(c, at_shard(q), shard)
            extra = recv_1[c, k].astype(F32)
            send_2[slot, k, k * part : (k + 1) * part] = (rows[k * part : (k + 1) * part] + extra).astype(BF16)
            send_2[slot, k, (1 - k) * part : (2 - k) * part] = rows[(1 - k) * part : (2 - k) * part].astype(BF16)
            second(c, slot, k).start()

    def finished(c, slot):
        for k in range(2):
            second(c, slot, k).wait()
        total = of_pair(c, at_shard(0), shard)
        total = (total + recv_2[c, 0].astype(F32) + recv_2[c, 1].astype(F32)).astype(BF16)
        red[slot] = total

        @pl.when(c < gathered)
        def _():
            spread(c, slot, 0).start()
            spread(c, slot, 1).start()

        kept(c, lambda which: keep(c, slot, which).start())
        total = total.astype(F32)
        squares[...] += jnp.sum((total * total).reshape(shard // 8, 8, CHUNK), 0)

    def kept(c, act):
        pl.when(c < gathered)(lambda: act(0))
        pl.when((c >= gathered) & (c < gathered + lows))(lambda: act(1))
        pl.when(c >= gathered + lows)(lambda: act(2))

    def spread_on(c, slot):
        kept(c, lambda which: keep(c, slot, which).wait())

        @pl.when(c < gathered)
        def _():
            for k in range(2):
                spread(c, slot, k).wait()
            for k in range(2):
                forward_on(c, k).start()

    def returned(c, slot):
        for k in range(2):
            forward_on(c, k).wait()
        pair_back(c).start()

    def serve_start(it):
        among(it - 3, 0, chunks, passed_on)
        among(it - 6, 0, chunks, spread_on)

    def serve_middle(it):
        among(it - 4, 0, chunks, finished)
        among(it - 1, 0, chunks, summed)
        among(it - 7, 0, gathered, returned)
        among(it - 8, 0, gathered, lambda c, slot: pair_back(c).wait())

    def step(it, _):
        if comm:
            serve_start(it)
        pl.when(it == (layers - 1) * per_layer)(next_layer)
        pl.when(it < chunks)(lambda: compute_hidden(it))
        if comm:
            serve_middle(it)
        pl.when(it < chunks)(lambda: compute_weights(it))
        if comm:
            pl.when(it < chunks)(lambda: pair(it, lax.rem(it, 2)).start())
        return 0

    lax.fori_loop(0, max(chunks + 7, gathered + 9) if comm else chunks, step, 0)

    if comm:
        all_squares[pl.ds(me, 1)] = squares[...][None]
        sends = [
            pltpu.make_async_remote_copy(
                src_ref=squares, dst_ref=all_squares.at[me], send_sem=norm_send.at[k], recv_sem=norm_recv.at[k],
                device_id={"dp": other}, device_id_type=pl.DeviceIdType.MESH,
            )
            for k, other in enumerate(others)
        ]
        for send in sends:
            send.start()
        for send in sends:
            send.wait()
        total = all_squares[0]
        for k in range(1, n):
            total += all_squares[k]
        norm_hbm[...] = total
    else:
        norm_hbm[...] = squares[...]
        pltpu.sync_copy(g.at[0], sum_hbm.at[0])


def train(n, x, h, dy, wg, wu, wd, gathered, comm=True):
    tokens, d = x.shape
    layers, _, ff = wg.shape
    per_layer = ff // CHUNK
    chunks, rows = layers * per_layer, 3 * d
    half = rows // 2
    shard = half // (n // 2)
    part = shard // 2
    lows = (chunks - gathered + 1) // 2
    hbm = pl.BlockSpec(memory_space=pl.ANY)
    vmem = pltpu.VMEM
    dma = pltpu.SemaphoreType.DMA
    return pl.pallas_call(
        functools.partial(train_kernel, n, layers, per_layer, gathered, comm),
        in_specs=[hbm] * 6,
        out_specs=[hbm, hbm, hbm, pl.BlockSpec(memory_space=pltpu.VMEM)],
        out_shape=[jax.ShapeDtypeStruct((k, r, CHUNK), BF16) for k, r in ((gathered, rows), (lows, shard), (chunks - gathered - lows, shard))]
        + [jax.ShapeDtypeStruct((8, CHUNK), F32)],
        scratch_shapes=[
            vmem((tokens, d), BF16), vmem((tokens, d), BF16), vmem((tokens, d), BF16), vmem((tokens, d), BF16), vmem((d, tokens), BF16), vmem((tokens, d), F32),
            vmem((2, d, 2 * CHUNK), BF16), vmem((2, CHUNK, d), BF16), vmem((tokens, CHUNK), BF16), vmem((tokens, 2 * CHUNK), BF16),
            vmem((4, rows, CHUNK), BF16),
            vmem((chunks, half, CHUNK), BF16), vmem((chunks, 2, part, CHUNK), BF16), vmem((chunks, 2, shard, CHUNK), BF16),
            vmem((2, 2, part, CHUNK), BF16), vmem((2, 2, shard, CHUNK), BF16), vmem((2, shard, CHUNK), BF16),
            vmem((8, CHUNK), F32), vmem((n, 8, CHUNK), F32),
            dma((3,)), dma((2, 3)), dma((chunks, 10)), dma((chunks, 10)), dma((chunks,)), dma((n - 1,)), dma((n - 1,)),
        ],
        compiler_params=pltpu.CompilerParams(collective_id=0 if comm else None, has_side_effects=True, vmem_limit_bytes=63 * 2**20),
        cost_estimate=pl.CostEstimate(flops=14 * tokens * d * ff * layers, bytes_accessed=60 * 2**20, transcendentals=0),
        name="train",
    )(x, h, dy, wg, wu, wd)


def adamw_kernel(count, pieces, squares_ref, *refs):
    w, m, v = (refs[pieces + i : pieces + i + 3] for i in (0, 3, 6))
    rest = refs[pieces + 9 :]
    if pieces == 1:
        g, rest = refs[0].at[0], rest[-9:]
    else:
        g, rest = rest[-1], rest[-10:-1]
        me = lax.axis_index("dp")
        chips, shard = pieces // 2, refs[0].shape[1]
        for i in range(pieces):
            core = (me + i // chips) % 2
            at = core * (chips * shard) + lax.rem(me // 2 + (0, chips - 1, 1, 2)[i % chips], chips) * shard
            g[pl.ds(pl.multiple_of(at, 16), shard), :] = refs[i][0]
    new_w, new_m, new_v = rest[:3], rest[3:6], rest[6:]
    total = jnp.sum(squares_ref[...], (0, 1), keepdims=True)
    factor = jnp.minimum(1.0, 0.5 * lax.rsqrt(total / count + 1e-30))
    d = w[0].shape[1]
    for i in range(3):
        if i < 2:
            grad = g[i * d : (i + 1) * d, :]
        else:
            grad = jnp.concatenate([g[2 * d + k : 2 * d + k + CHUNK, :] for k in range(0, d, CHUNK)], 1)
        grad = grad.astype(F32) * factor
        mean = 0.9 * m[i][0] + 0.1 * grad
        square = 0.95 * v[i][0] + 0.05 * grad * grad
        wide = w[i][0].astype(F32)
        new_w[i][0] = (wide - 0.02 * (mean * lax.rsqrt(square + 1e-8) + 0.1 * wide)).astype(BF16)
        new_m[i][0] = mean
        new_v[i][0] = square


def adamw(start, end, squares, gradients, weights, m, v, so_far):
    layers, d, ff = weights[0].shape
    per_layer = ff // CHUNK
    chunks, pieces = end - start, len(gradients)
    skip = start if pieces == 1 else 0
    layer = lambda i: layers - 1 - (start + i) // per_layer
    across = pl.BlockSpec((1, d, CHUNK), lambda i: (layer(i), 0, (start + i) % per_layer))
    down = pl.BlockSpec((1, CHUNK, d), lambda i: (layer(i), (start + i) % per_layer, 0))
    each = [across, across, down] * 3
    count = sum(w.size for w in weights)
    carried = list(so_far or [])
    return pl.pallas_call(
        functools.partial(adamw_kernel, count, pieces),
        grid=(chunks,),
        in_specs=[pl.BlockSpec((8, CHUNK), lambda i: (0, 0))]
        + [pl.BlockSpec((1, *g.shape[1:]), lambda i: (skip + i, 0, 0)) for g in gradients]
        + each
        + [pl.BlockSpec(memory_space=pl.ANY)] * len(carried),
        out_specs=each,
        out_shape=[jax.ShapeDtypeStruct(t.shape, t.dtype) for t in (*weights, *m, *v)],
        scratch_shapes=[] if pieces == 1 else [pltpu.VMEM((3 * d, CHUNK), BF16)],
        input_output_aliases={10 + pieces + i: i for i in range(len(carried))},
        compiler_params=pltpu.CompilerParams(dimension_semantics=("arbitrary",), vmem_limit_bytes=62 * 2**20),
        cost_estimate=pl.CostEstimate(flops=chunks * FLOPS_OF_A_CHUNK, bytes_accessed=chunks * 66 * d * CHUNK, transcendentals=0),
        name=f"adamw_{start}",
    )(squares, *gradients, *weights, *m, *v, *carried)


FLOPS_OF_A_CHUNK = 10**10


def solution(mesh):
    n = mesh.shape["dp"]
    chips = n // 2
    right = [(2 * c + k, (2 * c + 2) % n + k) for c in range(chips) for k in range(2)]
    left = [(to, source) for source, to in right]
    pairs = [(i, i ^ 1) for i in range(n)]

    def go(t, way):
        return lax.ppermute(t, "dp", way)

    def step(x, dy, *arrays):
        weights, m, v = (arrays[i : i + 3] for i in (0, 3, 6))
        h = forward(0, x[0], *weights)
        g, low, high, squares = train(n, x[0], h, dy[0], *weights, GATHERED)
        take = lambda first, end, parts, so_far: adamw(first, end, squares, parts, weights, m, v, so_far)
        lows = [low, go(low, right), go(low, left)]
        highs = [high, go(high, right), go(high, left)]
        low_pairs = [go(low, pairs)]
        high_pairs = [go(high, pairs)]
        new = take(0, GATHERED // 2, [g], None)
        lows, new = lax.optimization_barrier((lows, new))
        lows.append(go(lows[1], right))
        low_pairs += [go(t, pairs) for t in lows[1:3]]
        new = take(GATHERED // 2, GATHERED, [g], new)
        lows, highs, low_pairs, new = lax.optimization_barrier((lows, highs, low_pairs, new))
        highs.append(go(highs[2], left))
        low_pairs.append(go(lows[3], pairs))
        high_pairs += [go(t, pairs) for t in highs[1:3]]
        end = GATHERED + low.shape[0]
        new = take(GATHERED, end, lows + low_pairs, new)
        highs, high_pairs, new = lax.optimization_barrier((highs, high_pairs, new))
        high_pairs.append(go(highs[3], pairs))
        return tuple(take(end, end + high.shape[0], highs + high_pairs, new))

    return jax.shard_map(
        step,
        mesh=mesh,
        in_specs=(P(("rep", "dp"), None, None),) * 2 + (P(None, None, None),) * 9,
        out_specs=(P("rep", None, None),) * 9,
        check_vma=False,
    )
```
